32 devices in a mesh: dp: 8 (over z, y), tp: 4 (over x, core).
Axes of the slice: x: 2, y: 2, z: 4, core: 2. Of those that a mesh axis runs over, the one named last changes fastest.
Arguments:
- x_teach: bfloat16 [64, 256, 1024], P('dp', 'tp')
- x_stud: bfloat16 [64, 256, 312], P(('dp', 'tp'))
- w_up_t: bfloat16 [8, 1024, 4096], P(None, None, 'tp')
- w_down_t: bfloat16 [8, 4096, 1024], P(None, 'tp')
- gain_t: float32 [8, 1024], replicated
- head_t: bfloat16 [1024, 30592], P(None, 'tp')
- w_up_s: bfloat16 [2, 312, 1248], replicated
- w_down_s: bfloat16 [2, 1248, 312], replicated
- gain_s: float32 [2, 312], replicated
- proj_s: bfloat16 [2, 312, 1024], replicated
- head_s: bfloat16 [312, 30592], replicated
Outputs:
- output 1: float32 [], replicated
- output 2: float32 [2, 312, 1248], replicated
- output 3: float32 [2, 1248, 312], replicated
- output 4: float32 [2, 312], replicated
- output 5: float32 [2, 312, 1024], replicated
- output 6: float32 [312, 30592], replicated
All inputs are finite; a program needn't handle non-finite values.
Results may differ from the reference program's by a relative error of at most 0.00335172.
Values are sent between devices in bfloat16 or wider.
A program may use at most 1 GiB of HBM per device.

```python
import jax
import jax.numpy as jnp
from jax import lax

BATCH = 64
SEQ_LEN = 256
D_TEACH = 1024
D_STUD = 312
VOCAB_SIZE = 30592
FEAT_LAYERS = 2
TEACH_LAYERS = 8
NORM_EPS = 1e-6


def setup_inputs(seed: int = 0) -> dict:
    rng_keys = jax.random.split(jax.random.key(seed), 11)
    ff_teach = 4 * D_TEACH
    ff_stud = 4 * D_STUD

    def normal_bf16(rng_key, arr_shape, std_scale):
        return (jax.random.normal(rng_key, arr_shape, jnp.float32) * std_scale).astype(jnp.bfloat16)

    return {
        'x_teach': normal_bf16(rng_keys[0], (BATCH, SEQ_LEN, D_TEACH), 1.0),
        'x_stud': normal_bf16(rng_keys[1], (BATCH, SEQ_LEN, D_STUD), 1.0),
        'w_up_t': normal_bf16(rng_keys[2], (TEACH_LAYERS, D_TEACH, ff_teach), D_TEACH ** -0.5),
        'w_down_t': normal_bf16(rng_keys[3], (TEACH_LAYERS, ff_teach, D_TEACH), ff_teach ** -0.5),
        'gain_t': jax.random.uniform(rng_keys[4], (TEACH_LAYERS, D_TEACH), jnp.float32, 0.5, 1.5),
        'head_t': normal_bf16(rng_keys[5], (D_TEACH, VOCAB_SIZE), D_TEACH ** -0.5),
        'w_up_s': normal_bf16(rng_keys[6], (FEAT_LAYERS, D_STUD, ff_stud), D_STUD ** -0.5),
        'w_down_s': normal_bf16(rng_keys[7], (FEAT_LAYERS, ff_stud, D_STUD), ff_stud ** -0.5),
        'gain_s': jax.random.uniform(rng_keys[8], (FEAT_LAYERS, D_STUD), jnp.float32, 0.5, 1.5),
        'proj_s': normal_bf16(rng_keys[9], (FEAT_LAYERS, D_STUD, D_TEACH), D_STUD ** -0.5),
        'head_s': normal_bf16(rng_keys[10], (D_STUD, VOCAB_SIZE), D_STUD ** -0.5),
    }


def rms_norm(values):
    vals32 = values.astype(jnp.float32)
    return vals32 * lax.rsqrt(jnp.mean(vals32 * vals32, axis=-1, keepdims=True) + NORM_EPS)


def as_bf16(values):
    return values.astype(jnp.bfloat16).astype(jnp.float32)


def gelu_tanh(values):
    return jax.nn.gelu(values, approximate=True)


def teacher_tokens(teach_blk, w_up_t, w_down_t, gain_t, head_t):
    per_feat = TEACH_LAYERS // FEAT_LAYERS
    up_groups = w_up_t.reshape(FEAT_LAYERS, per_feat, D_TEACH, 4 * D_TEACH)
    down_groups = w_down_t.reshape(FEAT_LAYERS, per_feat, 4 * D_TEACH, D_TEACH)
    gain_groups = gain_t.reshape(FEAT_LAYERS, per_feat, D_TEACH)

    def one_layer(hidden, layer_w):
        w_up, w_down, gain_row = layer_w
        normed = (rms_norm(hidden) * gain_row).astype(jnp.bfloat16)
        hidden_act = gelu_tanh(jnp.dot(normed, w_up, preferred_element_type=jnp.float32)).astype(jnp.bfloat16)
        layer_out = jnp.dot(hidden_act, w_down, preferred_element_type=jnp.float32).astype(jnp.bfloat16)
        return hidden + layer_out, None

    def one_feature(hidden, group_w):
        hidden, _ = lax.scan(one_layer, hidden, group_w)
        return hidden, hidden

    hidden, features = lax.scan(one_feature, teach_blk, (up_groups, down_groups, gain_groups))
    teach_logits = jnp.dot(rms_norm(hidden).astype(jnp.bfloat16), head_t, preferred_element_type=jnp.float32)
    return features, teach_logits


def student_loss(params, stud_blk, features, teach_logits, feat_coef, kl_coef):
    w_up, w_down, gains, proj, head_w = params

    def one_block(residual, layer_w):
        up_j, down_j, gain_j, proj_j, feat_j = layer_w
        normed = as_bf16(rms_norm(residual) * gain_j)
        hidden_act = as_bf16(gelu_tanh(jnp.dot(normed, up_j, preferred_element_type=jnp.float32)))
        residual = residual + jnp.dot(hidden_act, down_j, preferred_element_type=jnp.float32)
        proj_in = as_bf16(rms_norm(residual))
        feat_err = jnp.dot(proj_in, proj_j, preferred_element_type=jnp.float32) - feat_j.astype(jnp.float32)
        return residual, jnp.sum(feat_err * feat_err)

    residual, err_sums = lax.scan(one_block, stud_blk.astype(jnp.float32), (w_up, w_down, gains, proj, features))
    stud_logits = jnp.dot(as_bf16(rms_norm(residual)), head_w, preferred_element_type=jnp.float32)
    log_teach = jax.nn.log_softmax(teach_logits, axis=-1)
    log_stud = jax.nn.log_softmax(stud_logits, axis=-1)
    kl_sum = jnp.sum(jnp.exp(log_teach) * (log_teach - log_stud))
    return feat_coef * jnp.sum(err_sums) + kl_coef * kl_sum


def reference(x_teach, x_stud, w_up_t, w_down_t, gain_t, head_t, w_up_s, w_down_s, gain_s, proj_s, head_s):
    block_len = 128
    n_tokens = BATCH * SEQ_LEN
    n_blocks = n_tokens // block_len
    teach_blocks = x_teach.reshape(n_blocks, block_len, D_TEACH)
    stud_blocks = x_stud.reshape(n_blocks, block_len, D_STUD)
    params = (w_up_s.astype(jnp.float32), w_down_s.astype(jnp.float32), gain_s.astype(jnp.float32),
              proj_s.astype(jnp.float32), head_s.astype(jnp.float32))
    feat_coef = 1.0 / (FEAT_LAYERS * n_tokens * D_TEACH)
    kl_coef = 1.0 / n_tokens
    loss_and_grad = jax.value_and_grad(student_loss)

    def one_block(scan_carry, token_blks):
        loss_acc, grad_acc = scan_carry
        teach_blk, stud_blk = token_blks
        features, teach_logits = teacher_tokens(teach_blk, w_up_t, w_down_t, gain_t, head_t)
        loss_val, grad_vals = loss_and_grad(params, stud_blk, features, teach_logits, feat_coef, kl_coef)
        return (loss_acc + loss_val, jax.tree.map(jnp.add, grad_acc, grad_vals)), None

    start_carry = (jnp.zeros((), jnp.float32), jax.tree.map(jnp.zeros_like, params))
    (total_loss, grad_vals), _ = lax.scan(one_block, start_carry, (teach_blocks, stud_blocks))
    grad_up, grad_down, grad_gain, grad_proj, grad_head = grad_vals
    return (total_loss, grad_up, grad_down, grad_gain, grad_proj, grad_head)
```

```python
import functools

import jax
import jax.numpy as jnp
from jax import lax
from jax.experimental import pallas as pl
from jax.experimental.pallas import tpu as pltpu
from jax.sharding import PartitionSpec as P

NORM_EPS = 1e-6


def rms_parts(values):
    vals32 = values.astype(jnp.float32)
    inv_rms = lax.rsqrt(jnp.mean(vals32 * vals32, axis=-1, keepdims=True) + NORM_EPS)
    return vals32 * inv_rms, inv_rms


def rms_back(normed, inv_rms, grad_out):
    return inv_rms * (grad_out - normed * jnp.mean(grad_out * normed, axis=-1, keepdims=True))


def gelu_tanh(values):
    return jax.nn.gelu(values, approximate=True)


def gelu_back(pre_act, grad_out):
    return jax.vjp(gelu_tanh, pre_act)[1](grad_out)[0]


def mat_mul(subscripts, lhs_arr, rhs_arr):
    return jnp.einsum(subscripts, lhs_arr, rhs_arr, preferred_element_type=jnp.float32)


def student_forward(x_stud, w_up_s, w_down_s, gain_s, proj_s, features):
    residual = x_stud.astype(jnp.float32)
    norm_cur, inv_cur = rms_parts(residual)
    saved_acts = []
    err_total = jnp.zeros((), jnp.float32)
    for layer_idx in range(w_up_s.shape[0]):
        normed = (norm_cur * gain_s[layer_idx]).astype(jnp.bfloat16)
        pre_act = mat_mul('bsd,df->bsf', normed, w_up_s[layer_idx])
        hidden_act = gelu_tanh(pre_act).astype(jnp.bfloat16)
        residual = residual + mat_mul('bsf,fd->bsd', hidden_act, w_down_s[layer_idx])
        norm_next, inv_next = rms_parts(residual)
        proj_in = norm_next.astype(jnp.bfloat16)
        feat_err = mat_mul('bsd,de->bse', proj_in, proj_s[layer_idx]) - features[layer_idx]
        err_total = err_total + jnp.sum(feat_err * feat_err)
        saved_acts.append((norm_cur, inv_cur, normed, pre_act, hidden_act, norm_next, inv_next, proj_in, feat_err))
        norm_cur, inv_cur = norm_next, inv_next
    return saved_acts, err_total


def student_backward(saved_acts, w_up_s, w_down_s, gain_s, proj_s, feat_coef, head_in_grad):
    n_layers = len(saved_acts)
    up_grads = []
    down_grads = []
    gain_grads = []
    proj_grads = []
    resid_grad = None
    for layer_idx in reversed(range(n_layers)):
        norm_cur, inv_cur, normed, pre_act, hidden_act, norm_next, inv_next, proj_in, feat_err = saved_acts[layer_idx]
        err_grad = (2.0 * feat_coef * feat_err).astype(jnp.bfloat16)
        proj_grads.append(mat_mul('bsd,bse->de', proj_in, err_grad))
        out_grad = mat_mul('bse,de->bsd', err_grad, proj_s[layer_idx])
        if resid_grad is None:
            resid_grad = rms_back(norm_next, inv_next, out_grad + head_in_grad)
        else:
            resid_grad = resid_grad + rms_back(norm_next, inv_next, out_grad)
        resid_bf = resid_grad.astype(jnp.bfloat16)
        down_grads.append(mat_mul('bsf,bsd->fd', hidden_act, resid_bf))
        act_grad = mat_mul('bsd,fd->bsf', resid_bf, w_down_s[layer_idx])
        pre_grad = gelu_back(pre_act, act_grad).astype(jnp.bfloat16)
        up_grads.append(mat_mul('bsd,bsf->df', normed, pre_grad))
        norm_grad = mat_mul('bsf,df->bsd', pre_grad, w_up_s[layer_idx])
        gain_grads.append(jnp.sum(norm_grad * norm_cur, axis=(0, 1)))
        if layer_idx > 0:
            resid_grad = resid_grad + rms_back(norm_cur, inv_cur, norm_grad * gain_s[layer_idx])
    return (jnp.stack(up_grads[::-1]), jnp.stack(down_grads[::-1]),
            jnp.stack(gain_grads[::-1]), jnp.stack(proj_grads[::-1]))


MESH = pl.DeviceIdType.MESH
N_DIRECT = 128
N_SEED = 112


def teacher_kernel(n_layers, x_ref, gain_ref, wu_ref, wd_ref, feat_ref, gu_ref, gd_ref,
                   h_ref, n_ref, a_ref, acc_ref, wb_ref, load_sem, send_sem, recv_sem):
    rows, d_model = x_ref.shape
    width = wu_ref.shape[2]
    per_feat = n_layers // feat_ref.shape[0]
    own = (wu_ref, wd_ref)
    got = (gu_ref, gd_ref)
    n_dir, n_seed = direct_rows(d_model), seed_rows(d_model)
    dp, tp = lax.axis_index('dp'), lax.axis_index('tp')
    z, y = dp // 2, dp % 2
    x, c = tp // 2, tp % 2
    zz = z % 2
    x_peer = (dp, (1 - x) * 2 + c)
    y_peer = (z * 2 + 1 - y, tp)
    z_peer = ((z + 1 - 2 * zz) * 2 + y, tp)
    mate = (dp, x * 2 + 1 - c)
    base_p, base_q = n_dir, n_dir + 4 * n_seed

    def rows_p(yy, zb):
        return pl.ds(pl.multiple_of(base_p + n_seed * (yy * 2 + zb), 16), n_seed)

    def rows_q(yy, zb):
        return pl.ds(pl.multiple_of(base_q + n_seed * (zb * 2 + yy), 16), n_seed)

    def pair_p(yy):
        return pl.ds(pl.multiple_of(base_p + 2 * n_seed * yy, 16), 2 * n_seed)

    def pair_q(zb):
        return pl.ds(pl.multiple_of(base_q + 2 * n_seed * zb, 16), 2 * n_seed)

    def copy(stage, l, m, src, dst, dev):
        t = 2 * l + m
        return pltpu.make_async_remote_copy(src, dst, send_sem.at[stage, t], recv_sem.at[stage, t],
                                            device_id=dev, device_id_type=MESH)

    def outgoing(stage, l, m):
        g, w = got[m], own[m]
        if stage == 0:
            r = rows_p(y, zz)
            return copy(0, l, m, w.at[l, r], g.at[1, l, r], x_peer)
        if stage == 1:
            r = rows_q(y, zz)
            return copy(1, l, m, w.at[l, r], g.at[1, l, r], x_peer)
        if stage == 2:
            r = pl.ds(0, n_dir)
            return copy(2, l, m, w.at[l, r], g.at[1, l, r], x_peer)
        if stage == 3:
            r = rows_p(y, zz)
            return copy(3, l, m, g.at[1, l, r], g.at[1, l, r], z_peer)
        if stage == 4:
            r = rows_q(y, zz)
            return copy(4, l, m, g.at[1, l, r], g.at[1, l, r], y_peer)
        if stage == 5:
            r = pair_p(y)
            return copy(5, l, m, g.at[1, l, r], g.at[1, l, r], y_peer)
        if stage == 6:
            r = pair_q(zz)
            return copy(6, l, m, g.at[1, l, r], g.at[1, l, r], z_peer)
        if stage == 7:
            return copy(7, l, m, w.at[l], g.at[0, l], mate)
        return copy(8, l, m, g.at[1, l], g.at[2, l], mate)

    def incoming(stage, l, m):
        g = got[m]
        r = (rows_p(y, zz), rows_q(y, zz), pl.ds(0, n_dir), rows_p(y, 1 - zz), rows_q(1 - y, zz),
             pair_p(1 - y), pair_q(1 - zz))
        if stage < 7:
            ref = g.at[1, l, r[stage]]
        else:
            ref = g.at[0, l] if stage == 7 else g.at[2, l]
        return copy(stage, l, m, ref, ref, mate)

    def send_x(l, m):
        for stage in (0, 1, 2):
            outgoing(stage, l, m).start()

    def hop_a(l, m):
        for stage, nxt in ((0, 3), (1, 4)):
            incoming(stage, l, m).wait_recv()
            outgoing(nxt, l, m).start()

    def hop_b(l, m):
        for stage, nxt in ((3, 5), (4, 6)):
            incoming(stage, l, m).wait_recv()
            outgoing(nxt, l, m).start()

    def hop_c(l, m):
        for stage in (2, 5, 6):
            incoming(stage, l, m).wait_recv()
        outgoing(8, l, m).start()

    def guarded(fn, l, m, limit):
        if isinstance(l, int):
            fn(l, m)
        else:
            pl.when(l < limit)(lambda: fn(l, m))

    def load(k, l, m):
        src = own[m].at[l] if k == 0 else got[m].at[k - 1, l]
        return pltpu.make_async_copy(src, wb_ref.at[k], load_sem.at[k])

    def normalize(l):
        def body(i, _):
            r = pl.ds(pl.multiple_of(i * 64, 64), 64)
            v = h_ref[r].astype(jnp.float32)
            v = v * lax.rsqrt(jnp.mean(v * v, axis=-1, keepdims=True) + NORM_EPS)
            n_ref[r] = (v * gain_ref[pl.ds(l, 1)]).astype(jnp.bfloat16)
            return 0
        lax.fori_loop(0, rows // 64, body, 0)

    tile = min(256, width)

    def up_part(k):
        def body(j, _):
            cols = pl.ds(pl.multiple_of(j * tile, tile), tile)
            u = jnp.dot(n_ref[...], wb_ref[k, :, cols], preferred_element_type=jnp.float32)
            a_ref[k, :, cols] = gelu_tanh(u).astype(jnp.bfloat16)
            return 0
        lax.fori_loop(0, width // tile, body, 0)

    def down_part(k):
        def body(j, _):
            cols = pl.ds(pl.multiple_of(j * tile, tile), tile)
            u = jnp.dot(a_ref[k], wb_ref[k, :, cols], preferred_element_type=jnp.float32)
            if k == 0:
                acc_ref[:, cols] = u
            else:
                acc_ref[:, cols] += u
            return 0
        lax.fori_loop(0, d_model // tile, body, 0)

    def residual():
        def body(i, _):
            r = pl.ds(pl.multiple_of(i * 64, 64), 64)
            h_ref[r] = h_ref[r] + acc_ref[r].astype(jnp.bfloat16)
            return 0
        lax.fori_loop(0, rows // 64, body, 0)

    def compute(l, m):
        incoming(7, l, m).wait_recv()
        load(1, l, m).start()
        load(2, l, m).start()
        if m == 0:
            normalize(l)
        for k in range(4):
            if k == 3:
                incoming(8, l, m).wait_recv()
                load(3, l, m).start()
            load(k, l, m).wait()
            (up_part, down_part)[m](k)
        if m == 1:
            residual()
            feat_ref[l // per_feat] = h_ref[...]

    barrier = pltpu.get_barrier_semaphore()
    for dev in (x_peer, y_peer, z_peer, mate):
        pl.semaphore_signal(barrier, inc=1, device_id=dev, device_id_type=MESH)
    h_ref[...] = x_ref[...]
    pl.semaphore_wait(barrier, 4)

    for l in range(3):
        for m in range(2):
            send_x(l, m)
            if l == 0:
                outgoing(7, l, m).start()
    load(0, 0, 0).start()
    hop_a(0, 0)
    hop_b(0, 0)
    hop_a(0, 1)
    hop_c(0, 0)
    hop_b(0, 1)
    hop_a(1, 0)

    def layer(l, _):
        for m in range(2):
            guarded(send_x, l + 3, m, n_layers)
            guarded(lambda a, b: outgoing(7, a, b).start(), l + 1, m, n_layers)
            nxt = (l, 1) if m == 0 else (l + 1, 0)
            guarded(hop_c, nxt[0], nxt[1], n_layers)
            compute(l, m)
            guarded(lambda a, b: load(0, a, b).start(), nxt[0], nxt[1], n_layers)
            guarded(hop_b, l + 1, m, n_layers)
            nxt = (l + 1, 1) if m == 0 else (l + 2, 0)
            guarded(hop_a, nxt[0], nxt[1], n_layers)
        return 0

    lax.fori_loop(0, n_layers, layer, 0)

    def drain(l, _):
        for m in range(2):
            for stage in range(9):
                outgoing(stage, l, m).wait_send()
        return 0

    lax.fori_loop(0, n_layers, drain, 0)


def direct_rows(d_model):
    return d_model - 8 * seed_rows(d_model)


def seed_rows(d_model):
    return max(16, (d_model // 9) // 16 * 16)


def run_teacher(x_teach, w_up_t, w_down_t, gain_t, n_feat):
    n_layers, d_model, width = w_up_t.shape
    rows = x_teach.shape[0] * x_teach.shape[1]
    x_flat = x_teach.reshape(rows, d_model)
    any_spec = pl.BlockSpec(memory_space=pl.ANY)
    vmem_spec = pl.BlockSpec(memory_space=pltpu.VMEM)
    n_ticks = 2 * n_layers
    feat, _, _ = pl.pallas_call(
        functools.partial(teacher_kernel, n_layers),
        name='teacher',
        out_shape=(jax.ShapeDtypeStruct((n_feat, rows, d_model), jnp.bfloat16),
                   jax.ShapeDtypeStruct((3, n_layers, d_model, width), jnp.bfloat16),
                   jax.ShapeDtypeStruct((3, n_layers, width, d_model), jnp.bfloat16)),
        in_specs=[vmem_spec, vmem_spec, any_spec, any_spec],
        out_specs=(vmem_spec, any_spec, any_spec),
        scratch_shapes=[
            pltpu.VMEM((rows, d_model), jnp.bfloat16),
            pltpu.VMEM((rows, d_model), jnp.bfloat16),
            pltpu.VMEM((4, rows, width), jnp.bfloat16),
            pltpu.VMEM((rows, d_model), jnp.float32),
            pltpu.VMEM((4, d_model, width), jnp.bfloat16),
            pltpu.SemaphoreType.DMA((4,)),
            pltpu.SemaphoreType.DMA((9, n_ticks)),
            pltpu.SemaphoreType.DMA((9, n_ticks)),
        ],
        compiler_params=pltpu.CompilerParams(collective_id=0, has_side_effects=True),
        cost_estimate=pl.CostEstimate(flops=2 * rows * d_model * width * 4 * 2 * n_layers,
                                      bytes_accessed=8 * n_layers * d_model * width * 2,
                                      transcendentals=rows * width * 4 * n_layers),
    )(x_flat, gain_t, w_up_t, w_down_t)
    return feat


def solution(mesh):
    dp_size = mesh.shape['dp']
    tp_size = mesh.shape['tp']

    def local_step(x_teach, x_stud, w_up_t, w_down_t, gain_t, head_t, w_up_s, w_down_s, gain_s, proj_s, head_s):
        n_feat = w_up_s.shape[0]
        feats = run_teacher(x_teach, w_up_t, w_down_t, gain_t, n_feat)
        features = [feats[i].reshape(x_teach.shape) for i in range(n_feat)]
        x_stud = lax.all_to_all(x_stud, 'tp', 1, 0, tiled=True)
        final_norm = rms_parts(features[-1])[0].astype(jnp.bfloat16)
        final_full = lax.all_gather(final_norm, 'tp', axis=0, tiled=True)
        teach_logits = mat_mul('bsd,dv->bsv', final_full, head_t)

        n_tokens = x_stud.shape[0] * x_stud.shape[1] * dp_size * tp_size
        feat_coef = 1.0 / (n_feat * n_tokens * head_t.shape[0])
        kl_coef = 1.0 / n_tokens
        saved_acts, err_total = student_forward(x_stud, w_up_s, w_down_s, gain_s, proj_s, features)
        head_in = saved_acts[-1][7]
        stud_full = lax.all_gather(head_in, 'tp', axis=0, tiled=True)
        vocab_part = head_t.shape[1]
        head_cols = lax.dynamic_slice_in_dim(head_s, lax.axis_index('tp') * vocab_part, vocab_part, axis=1)
        stud_logits = mat_mul('bsd,dv->bsv', stud_full, head_cols)
        peak_vals = lax.pmax(jnp.stack([jnp.max(teach_logits, axis=-1), jnp.max(stud_logits, axis=-1)]), 'tp')
        teach_exp = jnp.exp(teach_logits - peak_vals[0][..., None])
        stud_exp = jnp.exp(stud_logits - peak_vals[1][..., None])
        sum_vals = lax.psum(jnp.stack([jnp.sum(teach_exp, axis=-1), jnp.sum(stud_exp, axis=-1)]), 'tp')
        log_norms = peak_vals + jnp.log(sum_vals)
        teach_prob = teach_exp / sum_vals[0][..., None]
        stud_prob = stud_exp / sum_vals[1][..., None]
        log_ratio = teach_logits - stud_logits - (log_norms[0] - log_norms[1])[..., None]
        kl_local = jnp.sum(teach_prob * log_ratio)
        logit_grad = (kl_coef * (stud_prob - teach_prob)).astype(jnp.bfloat16)
        head_part = mat_mul('bsd,bsv->dv', stud_full, logit_grad)
        d_stud = head_s.shape[0]
        d_pad = -d_stud % (8 * dp_size)
        head_rows = lax.psum_scatter(jnp.pad(head_part, ((0, d_pad), (0, 0))), 'dp', scatter_dimension=0, tiled=True)
        head_all = lax.all_gather(head_rows, ('dp', 'tp'), axis=0, tiled=False)
        head_all = head_all.reshape(dp_size, tp_size, -1, vocab_part).transpose(0, 2, 1, 3)
        head_grad = head_all.reshape(d_stud + d_pad, tp_size * vocab_part)[:d_stud]
        full_in_grad = mat_mul('bsv,dv->bsd', logit_grad, head_cols)
        head_in_grad = lax.psum_scatter(full_in_grad, 'tp', scatter_dimension=0, tiled=True)
        local_grads = student_backward(saved_acts, w_up_s, w_down_s, gain_s, proj_s, feat_coef, head_in_grad)
        grad_up, grad_down, grad_gain, grad_proj = lax.psum(local_grads, ('dp', 'tp'))
        total_loss = lax.psum(feat_coef * err_total + kl_coef * kl_local, ('dp', 'tp'))
        return total_loss, grad_up, grad_down, grad_gain, grad_proj, head_grad

    in_specs = (P('dp', 'tp', None), P(('dp', 'tp'), None, None), P(None, None, 'tp'), P(None, 'tp', None),
                P(), P(None, 'tp'), P(), P(), P(), P(), P())
    out_specs = (P(), P(), P(), P(), P(), P())
    return jax.shard_map(local_step, mesh=mesh, in_specs=in_specs, out_specs=out_specs, check_vma=False)
```

```python
import functools

import jax
import jax.numpy as jnp
from jax import lax
from jax.experimental import pallas as pl
from jax.experimental.pallas import tpu as pltpu
from jax.sharding import PartitionSpec as P

NORM_EPS = 1e-6


def rms_parts(values):
    vals32 = values.astype(jnp.float32)
    inv_rms = lax.rsqrt(jnp.mean(vals32 * vals32, axis=-1, keepdims=True) + NORM_EPS)
    return vals32 * inv_rms, inv_rms


def rms_back(normed, inv_rms, grad_out):
    return inv_rms * (grad_out - normed * jnp.mean(grad_out * normed, axis=-1, keepdims=True))


def gelu_tanh(values):
    return jax.nn.gelu(values, approximate=True)


def gelu_back(pre_act, grad_out):
    return jax.vjp(gelu_tanh, pre_act)[1](grad_out)[0]


def mat_mul(subscripts, lhs_arr, rhs_arr):
    return jnp.einsum(subscripts, lhs_arr, rhs_arr, preferred_element_type=jnp.float32)


def student_forward(x_stud, w_up_s, w_down_s, gain_s, proj_s, features):
    residual = x_stud.astype(jnp.float32)
    norm_cur, inv_cur = rms_parts(residual)
    saved_acts = []
    err_total = jnp.zeros((), jnp.float32)
    for layer_idx in range(w_up_s.shape[0]):
        normed = (norm_cur * gain_s[layer_idx]).astype(jnp.bfloat16)
        pre_act = mat_mul('bsd,df->bsf', normed, w_up_s[layer_idx])
        hidden_act = gelu_tanh(pre_act).astype(jnp.bfloat16)
        residual = residual + mat_mul('bsf,fd->bsd', hidden_act, w_down_s[layer_idx])
        norm_next, inv_next = rms_parts(residual)
        proj_in = norm_next.astype(jnp.bfloat16)
        feat_err = mat_mul('bsd,de->bse', proj_in, proj_s[layer_idx]) - features[layer_idx]
        err_total = err_total + jnp.sum(feat_err * feat_err)
        saved_acts.append((norm_cur, inv_cur, normed, pre_act, hidden_act, norm_next, inv_next, proj_in, feat_err))
        norm_cur, inv_cur = norm_next, inv_next
    return saved_acts, err_total


def student_backward(saved_acts, w_up_s, w_down_s, gain_s, proj_s, feat_coef, head_in_grad):
    n_layers = len(saved_acts)
    up_grads = []
    down_grads = []
    gain_grads = []
    proj_grads = []
    resid_grad = None
    for layer_idx in reversed(range(n_layers)):
        norm_cur, inv_cur, normed, pre_act, hidden_act, norm_next, inv_next, proj_in, feat_err = saved_acts[layer_idx]
        err_grad = (2.0 * feat_coef * feat_err).astype(jnp.bfloat16)
        proj_grads.append(mat_mul('bsd,bse->de', proj_in, err_grad))
        out_grad = mat_mul('bse,de->bsd', err_grad, proj_s[layer_idx])
        if resid_grad is None:
            resid_grad = rms_back(norm_next, inv_next, out_grad + head_in_grad)
        else:
            resid_grad = resid_grad + rms_back(norm_next, inv_next, out_grad)
        resid_bf = resid_grad.astype(jnp.bfloat16)
        down_grads.append(mat_mul('bsf,bsd->fd', hidden_act, resid_bf))
        act_grad = mat_mul('bsd,fd->bsf', resid_bf, w_down_s[layer_idx])
        pre_grad = gelu_back(pre_act, act_grad).astype(jnp.bfloat16)
        up_grads.append(mat_mul('bsd,bsf->df', normed, pre_grad))
        norm_grad = mat_mul('bsf,df->bsd', pre_grad, w_up_s[layer_idx])
        gain_grads.append(jnp.sum(norm_grad * norm_cur, axis=(0, 1)))
        if layer_idx > 0:
            resid_grad = resid_grad + rms_back(norm_cur, inv_cur, norm_grad * gain_s[layer_idx])
    return (jnp.stack(up_grads[::-1]), jnp.stack(down_grads[::-1]),
            jnp.stack(gain_grads[::-1]), jnp.stack(proj_grads[::-1]))


MESH = pl.DeviceIdType.MESH
N_DIRECT = 128
N_SEED = 112


def teacher_kernel(n_layers, x_ref, gain_ref, wu_ref, wd_ref, feat_ref, gu_ref, gd_ref,
                   h_ref, n_ref, a_ref, acc_ref, wb_ref, load_sem, send_sem, recv_sem):
    rows, d_model = x_ref.shape
    width = wu_ref.shape[2]
    per_feat = n_layers // feat_ref.shape[0]
    own = (wu_ref, wd_ref)
    got = (gu_ref, gd_ref)
    n_dir, n_seed = direct_rows(d_model), seed_rows(d_model)
    dp, tp = lax.axis_index('dp'), lax.axis_index('tp')
    z, y = dp // 2, dp % 2
    x, c = tp // 2, tp % 2
    zz = z % 2
    x_peer = (dp, (1 - x) * 2 + c)
    y_peer = (z * 2 + 1 - y, tp)
    z_peer = ((z + 1 - 2 * zz) * 2 + y, tp)
    mate = (dp, x * 2 + 1 - c)
    base_p, base_q = n_dir, n_dir + 4 * n_seed

    def rows_p(yy, zb):
        return pl.ds(pl.multiple_of(base_p + n_seed * (yy * 2 + zb), 16), n_seed)

    def rows_q(yy, zb):
        return pl.ds(pl.multiple_of(base_q + n_seed * (zb * 2 + yy), 16), n_seed)

    def pair_p(yy):
        return pl.ds(pl.multiple_of(base_p + 2 * n_seed * yy, 16), 2 * n_seed)

    def pair_q(zb):
        return pl.ds(pl.multiple_of(base_q + 2 * n_seed * zb, 16), 2 * n_seed)

    def copy(stage, l, m, src, dst, dev):
        t = 2 * l + m
        return pltpu.make_async_remote_copy(src, dst, send_sem.at[stage, t], recv_sem.at[stage, t],
                                            device_id=dev, device_id_type=MESH)

    def outgoing(stage, l, m):
        g, w = got[m], own[m]
        if stage == 0:
            r = rows_p(y, zz)
            return copy(0, l, m, w.at[l, r], g.at[1, l, r], x_peer)
        if stage == 1:
            r = rows_q(y, zz)
            return copy(1, l, m, w.at[l, r], g.at[1, l, r], x_peer)
        if stage == 2:
            r = pl.ds(0, n_dir)
            return copy(2, l, m, w.at[l, r], g.at[1, l, r], x_peer)
        if stage == 3:
            r = rows_p(y, zz)
            return copy(3, l, m, g.at[1, l, r], g.at[1, l, r], z_peer)
        if stage == 4:
            r = rows_q(y, zz)
            return copy(4, l, m, g.at[1, l, r], g.at[1, l, r], y_peer)
        if stage == 5:
            r = pair_p(y)
            return copy(5, l, m, g.at[1, l, r], g.at[1, l, r], y_peer)
        if stage == 6:
            r = pair_q(zz)
            return copy(6, l, m, g.at[1, l, r], g.at[1, l, r], z_peer)
        if stage == 7:
            return copy(7, l, m, w.at[l], g.at[0, l], mate)
        return copy(8, l, m, g.at[1, l], g.at[2, l], mate)

    def incoming(stage, l, m):
        g = got[m]
        r = (rows_p(y, zz), rows_q(y, zz), pl.ds(0, n_dir), rows_p(y, 1 - zz), rows_q(1 - y, zz),
             pair_p(1 - y), pair_q(1 - zz))
        if stage < 7:
            ref = g.at[1, l, r[stage]]
        else:
            ref = g.at[0, l] if stage == 7 else g.at[2, l]
        return copy(stage, l, m, ref, ref, mate)

    def send_x(l, m):
        for stage in (0, 1, 2):
            outgoing(stage, l, m).start()

    def hop_a(l, m):
        for stage, nxt in ((0, 3), (1, 4)):
            incoming(stage, l, m).wait_recv()
            outgoing(nxt, l, m).start()

    def hop_b(l, m):
        for stage, nxt in ((3, 5), (4, 6)):
            incoming(stage, l, m).wait_recv()
            outgoing(nxt, l, m).start()

    def hop_c(l, m):
        for stage in (2, 5, 6):
            incoming(stage, l, m).wait_recv()
        outgoing(8, l, m).start()

    def guarded(fn, l, m, limit):
        if isinstance(l, int):
            fn(l, m)
        else:
            pl.when(l < limit)(lambda: fn(l, m))

    def load(k, l, m):
        src = own[m].at[l] if k == 0 else got[m].at[k - 1, l]
        return pltpu.make_async_copy(src, wb_ref.at[k], load_sem.at[k])

    def normalize(l):
        def body(i, _):
            r = pl.ds(pl.multiple_of(i * 64, 64), 64)
            v = h_ref[r].astype(jnp.float32)
            v = v * lax.rsqrt(jnp.mean(v * v, axis=-1, keepdims=True) + NORM_EPS)
            n_ref[r] = (v * gain_ref[pl.ds(l, 1)]).astype(jnp.bfloat16)
            return 0
        lax.fori_loop(0, rows // 64, body, 0)

    tile = min(256, width)

    def up_part(k):
        def body(j, _):
            cols = pl.ds(pl.multiple_of(j * tile, tile), tile)
            u = jnp.dot(n_ref[...], wb_ref[k, :, cols], preferred_element_type=jnp.float32)
            a_ref[k, :, cols] = gelu_tanh(u).astype(jnp.bfloat16)
            return 0
        lax.fori_loop(0, width // tile, body, 0)

    def down_part(k):
        def body(j, _):
            cols = pl.ds(pl.multiple_of(j * tile, tile), tile)
            u = jnp.dot(a_ref[k], wb_ref[k, :, cols], preferred_element_type=jnp.float32)
            if k == 0:
                acc_ref[:, cols] = u
            else:
                acc_ref[:, cols] += u
            return 0
        lax.fori_loop(0, d_model // tile, body, 0)

    def residual():
        def body(i, _):
            r = pl.ds(pl.multiple_of(i * 64, 64), 64)
            h_ref[r] = h_ref[r] + acc_ref[r].astype(jnp.bfloat16)
            return 0
        lax.fori_loop(0, rows // 64, body, 0)

    def compute(l, m):
        incoming(7, l, m).wait_recv()
        load(1, l, m).start()
        load(2, l, m).start()
        if m == 0:
            normalize(l)
        for k in range(4):
            if k == 3:
                incoming(8, l, m).wait_recv()
                load(3, l, m).start()
            load(k, l, m).wait()
            (up_part, down_part)[m](k)
        if m == 1:
            residual()
            feat_ref[l // per_feat] = h_ref[...]

    barrier = pltpu.get_barrier_semaphore()
    for dev in (x_peer, y_peer, z_peer, mate):
        pl.semaphore_signal(barrier, inc=1, device_id=dev, device_id_type=MESH)
    h_ref[...] = x_ref[...]
    pl.semaphore_wait(barrier, 4)

    for l in range(3):
        for m in range(2):
            send_x(l, m)
            if l == 0:
                outgoing(7, l, m).start()
    load(0, 0, 0).start()
    hop_a(0, 0)
    hop_b(0, 0)
    hop_a(0, 1)
    hop_c(0, 0)
    hop_b(0, 1)
    hop_a(1, 0)

    def layer(l, _):
        for m in range(2):
            guarded(send_x, l + 3, m, n_layers)
            guarded(lambda a, b: outgoing(7, a, b).start(), l + 1, m, n_layers)
            nxt = (l, 1) if m == 0 else (l + 1, 0)
            guarded(hop_c, nxt[0], nxt[1], n_layers)
            compute(l, m)
            guarded(lambda a, b: load(0, a, b).start(), nxt[0], nxt[1], n_layers)
            guarded(hop_b, l + 1, m, n_layers)
            nxt = (l + 1, 1) if m == 0 else (l + 2, 0)
            guarded(hop_a, nxt[0], nxt[1], n_layers)
        return 0

    lax.fori_loop(0, n_layers, layer, 0)

    def drain(l, _):
        for m in range(2):
            for stage in range(9):
                outgoing(stage, l, m).wait_send()
        return 0

    lax.fori_loop(0, n_layers, drain, 0)


def direct_rows(d_model):
    return d_model - 8 * seed_rows(d_model)


def seed_rows(d_model):
    return max(16, (d_model // 9) // 16 * 16)


def run_teacher(x_teach, w_up_t, w_down_t, gain_t, n_feat):
    n_layers, d_model, width = w_up_t.shape
    rows = x_teach.shape[0] * x_teach.shape[1]
    x_flat = x_teach.reshape(rows, d_model)
    any_spec = pl.BlockSpec(memory_space=pl.ANY)
    vmem_spec = pl.BlockSpec(memory_space=pltpu.VMEM)
    n_ticks = 2 * n_layers
    feat, _, _ = pl.pallas_call(
        functools.partial(teacher_kernel, n_layers),
        name='teacher',
        out_shape=(jax.ShapeDtypeStruct((n_feat, rows, d_model), jnp.bfloat16),
                   jax.ShapeDtypeStruct((3, n_layers, d_model, width), jnp.bfloat16),
                   jax.ShapeDtypeStruct((3, n_layers, width, d_model), jnp.bfloat16)),
        in_specs=[vmem_spec, vmem_spec, any_spec, any_spec],
        out_specs=(vmem_spec, any_spec, any_spec),
        scratch_shapes=[
            pltpu.VMEM((rows, d_model), jnp.bfloat16),
            pltpu.VMEM((rows, d_model), jnp.bfloat16),
            pltpu.VMEM((4, rows, width), jnp.bfloat16),
            pltpu.VMEM((rows, d_model), jnp.float32),
            pltpu.VMEM((4, d_model, width), jnp.bfloat16),
            pltpu.SemaphoreType.DMA((4,)),
            pltpu.SemaphoreType.DMA((9, n_ticks)),
            pltpu.SemaphoreType.DMA((9, n_ticks)),
        ],
        compiler_params=pltpu.CompilerParams(collective_id=0, has_side_effects=True),
        cost_estimate=pl.CostEstimate(flops=2 * rows * d_model * width * 4 * 2 * n_layers,
                                      bytes_accessed=8 * n_layers * d_model * width * 2,
                                      transcendentals=rows * width * 4 * n_layers),
    )(x_flat, gain_t, w_up_t, w_down_t)
    return feat


def head_chunk(vocab_part):
    return 512 if vocab_part > 4096 else 128


def stats_kernel(vocab_part, fn_ref, s_ref, wt_ref, ws_ref, st_ref, acct_ref, accs_ref,
                 mt_ref, zt_ref, ms_ref, zs_ref, w_ref):
    step = pl.program_id(0)
    n_steps = pl.num_programs(0)
    rows, chunk = fn_ref.shape[0], wt_ref.shape[1]
    blk = min(256, rows)

    @pl.when(step == 0)
    def _():
        for ref in (mt_ref, ms_ref):
            ref[...] = jnp.full_like(ref, -jnp.inf)
        for ref in (zt_ref, zs_ref, w_ref, acct_ref, accs_ref):
            ref[...] = jnp.zeros_like(ref)

    def run(masked):
        ws = ws_ref[...]
        if masked:
            valid = step * chunk + lax.broadcasted_iota(jnp.int32, (1, chunk), 1) < vocab_part
            ws = jnp.where(valid, ws.astype(jnp.float32), 0.0).astype(jnp.bfloat16)

        def fold(logits, r, m_ref, z_ref, acc_ref):
            m_old = m_ref[r]
            m_new = jnp.maximum(m_old, jnp.max(logits, axis=1, keepdims=True))
            scale = jnp.exp(m_old - m_new)
            e = jnp.exp(logits - m_new)
            m_ref[r] = m_new
            z_ref[r] = z_ref[r] * scale + jnp.sum(e, axis=1, keepdims=True)
            part = lax.dot_general(e.astype(jnp.bfloat16), ws, (((1,), (1,)), ((), ())),
                                   preferred_element_type=jnp.float32)
            acc_ref[r] = acc_ref[r] * scale + part
            return e, scale

        def body(i, _):
            r = pl.ds(pl.multiple_of(i * blk, blk), blk)
            lt = jnp.dot(fn_ref[r], wt_ref[...], preferred_element_type=jnp.float32)
            ls = jnp.dot(s_ref[r], ws, preferred_element_type=jnp.float32)
            diff = lt - ls
            if masked:
                diff = jnp.where(valid, diff, 0.0)
                lt = jnp.where(valid, lt, -jnp.inf)
                ls = jnp.where(valid, ls, -jnp.inf)
            e, scale = fold(lt, r, mt_ref, zt_ref, acct_ref)
            w_ref[r] = w_ref[r] * scale + jnp.sum(e * diff, axis=1, keepdims=True)
            fold(ls, r, ms_ref, zs_ref, accs_ref)
            return 0

        lax.fori_loop(0, rows // blk, body, 0)

    if vocab_part % chunk == 0:
        run(False)
    else:
        pl.when(step < n_steps - 1)(lambda: run(False))
        pl.when(step == n_steps - 1)(lambda: run(True))

    @pl.when(step == n_steps - 1)
    def _():
        lane = lax.broadcasted_iota(jnp.int32, st_ref.shape, 1)
        out = jnp.zeros(st_ref.shape, jnp.float32)
        for i, ref in enumerate((mt_ref, zt_ref, ms_ref, zs_ref, w_ref)):
            out = jnp.where(lane == i, ref[...], out)
        st_ref[...] = out


def head_stats(full_norm, stud_full, head_t, head_cols):
    rows, d_model = full_norm.shape
    d_stud = stud_full.shape[1]
    vocab_part = head_t.shape[1]
    chunk = head_chunk(vocab_part)
    n_steps = pl.cdiv(vocab_part, chunk)
    whole = lambda shape: pl.BlockSpec(shape, lambda i: (0, 0), pipeline_mode=pl.Buffered(1))
    return pl.pallas_call(
        functools.partial(stats_kernel, vocab_part),
        name='head_stats',
        grid=(n_steps,),
        out_shape=(jax.ShapeDtypeStruct((rows, 128), jnp.float32),
                   jax.ShapeDtypeStruct((rows, d_stud), jnp.float32),
                   jax.ShapeDtypeStruct((rows, d_stud), jnp.float32)),
        in_specs=[whole((rows, d_model)), whole((rows, d_stud)),
                  pl.BlockSpec((d_model, chunk), lambda i: (0, i)),
                  pl.BlockSpec((d_stud, chunk), lambda i: (0, i))],
        out_specs=(whole((rows, 128)), whole((rows, d_stud)), whole((rows, d_stud))),
        scratch_shapes=[pltpu.VMEM((rows, 1), jnp.float32)] * 5,
        cost_estimate=pl.CostEstimate(flops=2 * rows * vocab_part * (d_model + 3 * d_stud),
                                      bytes_accessed=2 * vocab_part * (d_model + d_stud),
                                      transcendentals=2 * rows * vocab_part),
    )(full_norm, stud_full, head_t, head_cols)


HEAD_STAGES = 9


def head_grad_kernel(vocab_part, n_chunks, kl_coef, fn_ref, s_ref, st_ref, lt_ref, ls_ref, wt_ref, ws_ref, out_ref,
                     d_ref, part_ref, yb_ref, nb_ref, fb_ref, copy_sem, send_sem, recv_sem):
    step = pl.program_id(0)
    rows, chunk = fn_ref.shape[0], wt_ref.shape[1]
    d_stud = st_ref.shape[0]
    d_pad = part_ref.shape[1]
    half, quart, eighth = d_pad // 2, d_pad // 4, d_pad // 8
    blk = min(256, rows)
    dp, tp = lax.axis_index('dp'), lax.axis_index('tp')
    z, y = dp // 2, dp % 2
    x, c = tp // 2, tp % 2
    zz, zh = z % 2, z // 2
    tp_x = (1 - x) * 2 + c
    x_peer = (dp, tp_x)
    mate = (dp, x * 2 + 1 - c)
    y_peer = (z * 2 + 1 - y, tp)
    near = ((z + 1 - 2 * zz) * 2 + y, tp)
    far = (((1 - zh) * 2 + zz) * 2 + y, tp)

    def span(yy, n=None, f=None):
        start, size = yy * half, half
        if n is not None:
            start, size = start + n * quart, quart
        if f is not None:
            start, size = start + f * eighth, eighth
        return pl.ds(pl.multiple_of(start, 8), size)

    def cols(i):
        return pl.ds(pl.multiple_of(i * chunk, chunk), chunk)

    def copy(stage, i, src, dst, dev):
        return pltpu.make_async_remote_copy(src, dst, send_sem.at[stage, i], recv_sem.at[stage, i],
                                            device_id=dev, device_id_type=MESH)

    def outgoing(stage, i):
        g = out_ref.at[tp]
        if stage == 0:
            return copy(0, i, part_ref.at[i, span(1 - y)], yb_ref.at[i], y_peer)
        if stage == 1:
            return copy(1, i, part_ref.at[i, span(y, 1 - zz)], nb_ref.at[i], near)
        if stage == 2:
            return copy(2, i, part_ref.at[i, span(y, zz, 1 - zh)], fb_ref.at[i], far)
        if stage == 3:
            r = span(y, zz, zh)
            return copy(3, i, part_ref.at[i, r], g.at[r, cols(i)], far)
        if stage == 4:
            r = span(y, zz)
            return copy(4, i, g.at[r, cols(i)], g.at[r, cols(i)], near)
        if stage == 5:
            r = span(y)
            return copy(5, i, g.at[r, cols(i)], g.at[r, cols(i)], y_peer)
        if stage == 6:
            return copy(6, i, g.at[:, cols(i)], g.at[:, cols(i)], x_peer)
        if stage == 7:
            return copy(7, i, g.at[:, cols(i)], g.at[:, cols(i)], mate)
        gx = out_ref.at[tp_x]
        return copy(8, i, gx.at[:, cols(i)], gx.at[:, cols(i)], mate)

    def incoming(stage, i):
        g = out_ref.at[tp]
        if stage < 3:
            ref = (yb_ref, nb_ref, fb_ref)[stage].at[i]
        elif stage < 6:
            r = (span(y, zz, 1 - zh), span(y, 1 - zz), span(1 - y))[stage - 3]
            ref = g.at[r, cols(i)]
        elif stage == 6:
            ref = out_ref.at[tp_x, :, cols(i)]
        elif stage == 7:
            ref = out_ref.at[x * 2 + 1 - c, :, cols(i)]
        else:
            ref = out_ref.at[(1 - x) * 2 + 1 - c, :, cols(i)]
        return copy(stage, i, ref, ref, mate)

    def keep(i):
        r = span(y, zz, zh)
        return pltpu.make_async_copy(part_ref.at[i, r], out_ref.at[tp, r, cols(i)], copy_sem.at[i])

    def compute(masked):
        if masked:
            valid = step * chunk + lax.broadcasted_iota(jnp.int32, (1, chunk), 1) < vocab_part

        def body(i, _):
            r = pl.ds(pl.multiple_of(i * blk, blk), blk)
            lt = jnp.dot(fn_ref[r], wt_ref[...], preferred_element_type=jnp.float32)
            ls = jnp.dot(s_ref[r], ws_ref[...], preferred_element_type=jnp.float32)
            shift_t = jnp.concatenate([lt_ref[r]] * (chunk // 128), axis=1)
            shift_s = jnp.concatenate([ls_ref[r]] * (chunk // 128), axis=1)
            diff = kl_coef * (jnp.exp(ls - shift_s) - jnp.exp(lt - shift_t))
            if masked:
                diff = jnp.where(valid, diff, 0.0)
            d_ref[r] = diff.astype(jnp.bfloat16)
            return 0

        lax.fori_loop(0, rows // blk, body, 0)
        grad = jnp.dot(st_ref[...], d_ref[...], preferred_element_type=jnp.float32)
        part_ref[step, pl.ds(0, d_stud)] = grad
        if d_pad > d_stud:
            part_ref[step, pl.ds(d_stud, d_pad - d_stud)] = jnp.zeros((d_pad - d_stud, chunk), jnp.float32)

    @pl.when(step == 0)
    def _():
        barrier = pltpu.get_barrier_semaphore()
        for dev in (x_peer, y_peer, near, far, mate):
            pl.semaphore_signal(barrier, inc=1, device_id=dev, device_id_type=MESH)
        pl.semaphore_wait(barrier, 5)

    if vocab_part % chunk == 0:
        pl.when(step < n_chunks)(lambda: compute(False))
    else:
        pl.when(step < n_chunks - 1)(lambda: compute(False))
        pl.when(step == n_chunks - 1)(lambda: compute(True))

    def lagged(lag, fn):
        i = step - lag
        pl.when((i >= 0) & (i < n_chunks))(lambda: fn(i))

    def add(stage, rng, buf):
        def fn(i):
            incoming(stage, i).wait_recv()
            part_ref[i, rng] += buf[i]
        return fn

    lagged(1, add(0, span(y), yb_ref))
    lagged(2, add(1, span(y, zz), nb_ref))
    lagged(3, add(2, span(y, zz, zh), fb_ref))

    def start_y(i):
        outgoing(0, i).start()

    def start_near(i):
        outgoing(1, i).start()

    def start_far(i):
        outgoing(2, i).start()

    def start_back_far(i):
        outgoing(3, i).start()
        keep(i).start()

    def start_back_near(i):
        incoming(3, i).wait_recv()
        keep(i).wait()
        outgoing(4, i).start()

    def start_back_y(i):
        incoming(4, i).wait_recv()
        outgoing(5, i).start()

    def start_out(i):
        incoming(5, i).wait_recv()
        outgoing(6, i).start()
        outgoing(7, i).start()

    def start_relay(i):
        incoming(6, i).wait_recv()
        outgoing(8, i).start()

    def finish(i):
        incoming(7, i).wait_recv()
        incoming(8, i).wait_recv()

    for lag, fn in ((0, start_y), (1, start_near), (2, start_far), (3, start_back_far), (4, start_back_near),
                    (5, start_back_y), (6, start_out), (7, start_relay), (8, finish)):
        lagged(lag, fn)

    @pl.when(step == pl.num_programs(0) - 1)
    def _():
        def drain(i, _):
            for stage in range(HEAD_STAGES):
                outgoing(stage, i).wait_send()
            return 0
        lax.fori_loop(0, n_chunks, drain, 0)


def head_grads(full_norm, stud_full, log_t, log_s, head_t, head_cols, kl_coef, tp_size):
    rows, d_model = full_norm.shape
    d_stud = stud_full.shape[1]
    vocab_part = head_t.shape[1]
    chunk = head_chunk(vocab_part)
    n_chunks = pl.cdiv(vocab_part, chunk)
    d_pad = pl.cdiv(d_stud, 64) * 64
    whole = lambda shape: pl.BlockSpec(shape, lambda i: (0, 0), pipeline_mode=pl.Buffered(1))
    return pl.pallas_call(
        functools.partial(head_grad_kernel, vocab_part, n_chunks, kl_coef),
        name='head_grads',
        grid=(n_chunks + 9,),
        out_shape=jax.ShapeDtypeStruct((tp_size, d_pad, n_chunks * chunk), jnp.float32),
        in_specs=[whole((rows, d_model)), whole((rows, d_stud)), whole((d_stud, rows)),
                  whole((rows, 128)), whole((rows, 128)),
                  pl.BlockSpec((d_model, chunk), lambda i: (0, jnp.minimum(i, n_chunks - 1))),
                  pl.BlockSpec((d_stud, chunk), lambda i: (0, jnp.minimum(i, n_chunks - 1)))],
        out_specs=pl.BlockSpec(memory_space=pl.ANY),
        scratch_shapes=[
            pltpu.VMEM((rows, chunk), jnp.bfloat16),
            pltpu.VMEM((n_chunks, d_pad, chunk), jnp.float32),
            pltpu.VMEM((n_chunks, d_pad // 2, chunk), jnp.float32),
            pltpu.VMEM((n_chunks, d_pad // 4, chunk), jnp.float32),
            pltpu.VMEM((n_chunks, d_pad // 8, chunk), jnp.float32),
            pltpu.SemaphoreType.DMA((n_chunks,)),
            pltpu.SemaphoreType.DMA((HEAD_STAGES, n_chunks)),
            pltpu.SemaphoreType.DMA((HEAD_STAGES, n_chunks)),
        ],
        compiler_params=pltpu.CompilerParams(collective_id=1, has_side_effects=True),
        cost_estimate=pl.CostEstimate(flops=200 * 10**9, bytes_accessed=2 * vocab_part * (d_model + d_stud),
                                      transcendentals=2 * rows * vocab_part),
    )(full_norm, stud_full, stud_full.T, jnp.broadcast_to(log_t[:, None], (rows, 128)),
      jnp.broadcast_to(log_s[:, None], (rows, 128)), head_t, head_cols)


def join_kernel(vocab_part, in_ref, out_ref):
    out_ref[...] = jnp.concatenate([in_ref[q, :, :vocab_part] for q in range(in_ref.shape[0])], axis=1)


def join_quarters(parts, d_stud, vocab_part):
    n_parts, _, padded = parts.shape
    blk = 24 if d_stud % 24 == 0 else 8
    return pl.pallas_call(
        functools.partial(join_kernel, vocab_part),
        name='join_quarters',
        grid=(d_stud // blk,),
        out_shape=jax.ShapeDtypeStruct((d_stud, n_parts * vocab_part), jnp.float32),
        in_specs=[pl.BlockSpec((n_parts, blk, padded), lambda i: (0, i, 0))],
        out_specs=pl.BlockSpec((blk, n_parts * vocab_part), lambda i: (i, 0)),
        cost_estimate=pl.CostEstimate(flops=d_stud * n_parts * vocab_part, transcendentals=0,
                                      bytes_accessed=8 * d_stud * n_parts * vocab_part),
    )(parts)


def solution(mesh):
    dp_size = mesh.shape['dp']
    tp_size = mesh.shape['tp']

    def local_step(x_teach, x_stud, w_up_t, w_down_t, gain_t, head_t, w_up_s, w_down_s, gain_s, proj_s, head_s):
        n_feat = w_up_s.shape[0]
        feats = run_teacher(x_teach, w_up_t, w_down_t, gain_t, n_feat)
        features = [feats[i].reshape(x_teach.shape) for i in range(n_feat)]
        x_stud = lax.all_to_all(x_stud, 'tp', 1, 0, tiled=True)
        final_norm = rms_parts(features[-1])[0].astype(jnp.bfloat16)
        final_full = lax.all_gather(final_norm, 'tp', axis=0, tiled=True)
        teach_logits = mat_mul('bsd,dv->bsv', final_full, head_t)

        n_tokens = x_stud.shape[0] * x_stud.shape[1] * dp_size * tp_size
        feat_coef = 1.0 / (n_feat * n_tokens * head_t.shape[0])
        kl_coef = 1.0 / n_tokens
        saved_acts, err_total = student_forward(x_stud, w_up_s, w_down_s, gain_s, proj_s, features)
        d_stud, d_teach = x_stud.shape[2], x_teach.shape[2]
        vocab_part = head_t.shape[1]
        n_own = x_stud.shape[0] * x_stud.shape[1]
        tp_idx = lax.axis_index('tp')
        head_in = saved_acts[-1][7]
        stud_full = lax.all_gather(head_in, 'tp', axis=0, tiled=True).reshape(tp_size * n_own, d_stud)
        full_norm = final_full.reshape(tp_size * n_own, d_teach)
        head_cols = lax.dynamic_slice_in_dim(head_s, tp_idx * vocab_part, vocab_part, axis=1)
        stats, acc_t, acc_s = head_stats(full_norm, stud_full, head_t, head_cols)
        all_stats = lax.all_gather(stats[:, :5].T, 'tp', axis=0)
        peaks = jnp.max(all_stats[:, 0::2][:, :2], axis=0)
        scales = jnp.exp(all_stats[:, 0:4:2] - peaks)
        sums = jnp.sum(all_stats[:, 1:4:2] * scales, axis=0)
        log_norms = peaks + jnp.log(sums)
        kl_tokens = (jnp.sum(all_stats[:, 4] * scales[:, 0], axis=0) / sums[0]) - (log_norms[0] - log_norms[1])
        kl_local = jnp.sum(lax.dynamic_slice_in_dim(kl_tokens, tp_idx * n_own, n_own))
        own_t = jnp.exp(stats[:, 0] - log_norms[0])[:, None]
        own_s = jnp.exp(stats[:, 2] - log_norms[1])[:, None]
        full_in_grad = kl_coef * (acc_s * own_s - acc_t * own_t)
        head_in_grad = lax.psum_scatter(full_in_grad, 'tp', scatter_dimension=0, tiled=True).reshape(x_stud.shape)
        grad_up, grad_down, grad_gain, grad_proj = student_backward(
            saved_acts, w_up_s, w_down_s, gain_s, proj_s, feat_coef, head_in_grad)
        loss_part = feat_coef * err_total + kl_coef * kl_local
        extra = jnp.stack([grad_gain, jnp.full_like(grad_gain, loss_part)], axis=-1)
        packed = jnp.concatenate([grad_proj, extra], axis=-1)
        log_norms, grad_up, grad_down, packed = lax.optimization_barrier((log_norms, grad_up, grad_down, packed))
        grad_up, grad_down, packed = lax.psum((grad_up, grad_down, packed), ('dp', 'tp'))
        parts = head_grads(full_norm, stud_full, log_norms[0], log_norms[1], head_t, head_cols, kl_coef, tp_size)
        head_grad = join_quarters(parts, d_stud, vocab_part)
        grad_proj, grad_gain = packed[..., :d_teach], packed[..., d_teach]
        total_loss = packed[0, 0, d_teach + 1]
        return total_loss, grad_up, grad_down, grad_gain, grad_proj, head_grad

    in_specs = (P('dp', 'tp', None), P(('dp', 'tp'), None, None), P(None, None, 'tp'), P(None, 'tp', None),
                P(), P(None, 'tp'), P(), P(), P(), P(), P())
    out_specs = (P(), P(), P(), P(), P(), P())
    return jax.shard_map(local_step, mesh=mesh, in_specs=in_specs, out_specs=out_specs, check_vma=False)
```

```python
import functools

import jax
import jax.numpy as jnp
from jax import lax
from jax.experimental import pallas as pl
from jax.experimental.pallas import tpu as pltpu
from jax.sharding import PartitionSpec as P

NORM_EPS = 1e-6


def rms_parts(values):
    vals32 = values.astype(jnp.float32)
    inv_rms = lax.rsqrt(jnp.mean(vals32 * vals32, axis=-1, keepdims=True) + NORM_EPS)
    return vals32 * inv_rms, inv_rms


def rms_back(normed, inv_rms, grad_out):
    return inv_rms * (grad_out - normed * jnp.mean(grad_out * normed, axis=-1, keepdims=True))


def gelu_tanh(values):
    return jax.nn.gelu(values, approximate=True)


def gelu_back(pre_act, grad_out):
    return jax.vjp(gelu_tanh, pre_act)[1](grad_out)[0]


def mat_mul(subscripts, lhs_arr, rhs_arr):
    return jnp.einsum(subscripts, lhs_arr, rhs_arr, preferred_element_type=jnp.float32)


def student_forward(x_stud, w_up_s, w_down_s, gain_s):
    residual = x_stud.astype(jnp.float32)
    norm_cur, inv_cur = rms_parts(residual)
    saved_acts = []
    for layer_idx in range(w_up_s.shape[0]):
        normed = (norm_cur * gain_s[layer_idx]).astype(jnp.bfloat16)
        pre_act = mat_mul('bsd,df->bsf', normed, w_up_s[layer_idx])
        hidden_act = gelu_tanh(pre_act).astype(jnp.bfloat16)
        residual = residual + mat_mul('bsf,fd->bsd', hidden_act, w_down_s[layer_idx])
        norm_next, inv_next = rms_parts(residual)
        proj_in = norm_next.astype(jnp.bfloat16)
        saved_acts.append((norm_cur, inv_cur, normed, pre_act, hidden_act, norm_next, inv_next, proj_in))
        norm_cur, inv_cur = norm_next, inv_next
    return saved_acts


def student_errors(saved_acts, proj_s, features, feat_coef):
    err_total = jnp.zeros((), jnp.float32)
    err_grads = []
    proj_grads = []
    for layer_idx, acts in enumerate(saved_acts):
        proj_in = acts[7]
        feat_err = mat_mul('bsd,de->bse', proj_in, proj_s[layer_idx]) - features[layer_idx]
        err_total = err_total + jnp.sum(feat_err * feat_err)
        err_grad = (2.0 * feat_coef * feat_err).astype(jnp.bfloat16)
        proj_grads.append(mat_mul('bsd,bse->de', proj_in, err_grad))
        err_grads.append(err_grad)
    return err_grads, err_total, jnp.stack(proj_grads)


def student_backward(saved_acts, w_up_s, w_down_s, gain_s, proj_s, err_grads, head_in_grad):
    n_layers = len(saved_acts)
    up_grads = []
    down_grads = []
    gain_grads = []
    resid_grad = None
    for layer_idx in reversed(range(n_layers)):
        norm_cur, inv_cur, normed, pre_act, hidden_act, norm_next, inv_next, proj_in = saved_acts[layer_idx]
        out_grad = mat_mul('bse,de->bsd', err_grads[layer_idx], proj_s[layer_idx])
        if resid_grad is None:
            resid_grad = rms_back(norm_next, inv_next, out_grad + head_in_grad)
        else:
            resid_grad = resid_grad + rms_back(norm_next, inv_next, out_grad)
        resid_bf = resid_grad.astype(jnp.bfloat16)
        down_grads.append(mat_mul('bsf,bsd->fd', hidden_act, resid_bf))
        act_grad = mat_mul('bsd,fd->bsf', resid_bf, w_down_s[layer_idx])
        pre_grad = gelu_back(pre_act, act_grad).astype(jnp.bfloat16)
        up_grads.append(mat_mul('bsd,bsf->df', normed, pre_grad))
        norm_grad = mat_mul('bsf,df->bsd', pre_grad, w_up_s[layer_idx])
        gain_grads.append(jnp.sum(norm_grad * norm_cur, axis=(0, 1)))
        if layer_idx > 0:
            resid_grad = resid_grad + rms_back(norm_cur, inv_cur, norm_grad * gain_s[layer_idx])
    return jnp.stack(up_grads[::-1]), jnp.stack(down_grads[::-1]), jnp.stack(gain_grads[::-1])


MESH = pl.DeviceIdType.MESH
N_DIRECT = 128
N_SEED = 112


def stud_chunk(vocab):
    return 2048 if vocab > 16384 else 256


def teacher_kernel(n_layers, x_ref, gain_ref, s_ref, wu_ref, wd_ref, hs_ref, feat_ref, lse_ref, ds_ref, gu_ref, gd_ref,
                   h_ref, n_ref, a_ref, acc_ref, wb_ref, hb_ref, m_ref, z_ref, load_sem, hs_sem, send_sem, recv_sem):
    rows, d_model = x_ref.shape
    width = wu_ref.shape[2]
    per_feat = n_layers // feat_ref.shape[0]
    own = (wu_ref, wd_ref)
    got = (gu_ref, gd_ref)
    n_dir, n_seed = direct_rows(d_model), seed_rows(d_model)
    dp, tp = lax.axis_index('dp'), lax.axis_index('tp')
    z, y = dp // 2, dp % 2
    x, c = tp // 2, tp % 2
    zz = z % 2
    x_peer = (dp, (1 - x) * 2 + c)
    y_peer = (z * 2 + 1 - y, tp)
    z_peer = ((z + 1 - 2 * zz) * 2 + y, tp)
    mate = (dp, x * 2 + 1 - c)
    base_p, base_q = n_dir, n_dir + 4 * n_seed

    def rows_p(yy, zb):
        return pl.ds(pl.multiple_of(base_p + n_seed * (yy * 2 + zb), 16), n_seed)

    def rows_q(yy, zb):
        return pl.ds(pl.multiple_of(base_q + n_seed * (zb * 2 + yy), 16), n_seed)

    def pair_p(yy):
        return pl.ds(pl.multiple_of(base_p + 2 * n_seed * yy, 16), 2 * n_seed)

    def pair_q(zb):
        return pl.ds(pl.multiple_of(base_q + 2 * n_seed * zb, 16), 2 * n_seed)

    def copy(stage, l, m, src, dst, dev):
        t = 2 * l + m
        return pltpu.make_async_remote_copy(src, dst, send_sem.at[stage, t], recv_sem.at[stage, t],
                                            device_id=dev, device_id_type=MESH)

    def outgoing(stage, l, m):
        g, w = got[m], own[m]
        if stage == 0:
            r = rows_p(y, zz)
            return copy(0, l, m, w.at[l, r], g.at[1, l, r], x_peer)
        if stage == 1:
            r = rows_q(y, zz)
            return copy(1, l, m, w.at[l, r], g.at[1, l, r], x_peer)
        if stage == 2:
            r = pl.ds(0, n_dir)
            return copy(2, l, m, w.at[l, r], g.at[1, l, r], x_peer)
        if stage == 3:
            r = rows_p(y, zz)
            return copy(3, l, m, g.at[1, l, r], g.at[1, l, r], z_peer)
        if stage == 4:
            r = rows_q(y, zz)
            return copy(4, l, m, g.at[1, l, r], g.at[1, l, r], y_peer)
        if stage == 5:
            r = pair_p(y)
            return copy(5, l, m, g.at[1, l, r], g.at[1, l, r], y_peer)
        if stage == 6:
            r = pair_q(zz)
            return copy(6, l, m, g.at[1, l, r], g.at[1, l, r], z_peer)
        if stage == 7:
            return copy(7, l, m, w.at[l], g.at[0, l], mate)
        return copy(8, l, m, g.at[1, l], g.at[2, l], mate)

    def incoming(stage, l, m):
        g = got[m]
        r = (rows_p(y, zz), rows_q(y, zz), pl.ds(0, n_dir), rows_p(y, 1 - zz), rows_q(1 - y, zz),
             pair_p(1 - y), pair_q(1 - zz))
        if stage < 7:
            ref = g.at[1, l, r[stage]]
        else:
            ref = g.at[0, l] if stage == 7 else g.at[2, l]
        return copy(stage, l, m, ref, ref, mate)

    def send_x(l, m):
        for stage in (0, 1, 2):
            outgoing(stage, l, m).start()

    def hop_a(l, m):
        for stage, nxt in ((0, 3), (1, 4)):
            incoming(stage, l, m).wait_recv()
            outgoing(nxt, l, m).start()

    def hop_b(l, m):
        for stage, nxt in ((3, 5), (4, 6)):
            incoming(stage, l, m).wait_recv()
            outgoing(nxt, l, m).start()

    def hop_c(l, m):
        for stage in (2, 5, 6):
            incoming(stage, l, m).wait_recv()
        outgoing(8, l, m).start()

    def guarded(fn, l, m, limit):
        if isinstance(l, int):
            fn(l, m)
        else:
            pl.when(l < limit)(lambda: fn(l, m))

    def load(k, l, m):
        src = own[m].at[l] if k == 0 else got[m].at[k - 1, l]
        return pltpu.make_async_copy(src, wb_ref.at[k], load_sem.at[k])

    def normalize(l):
        def body(i, _):
            r = pl.ds(pl.multiple_of(i * 64, 64), 64)
            v = h_ref[r].astype(jnp.float32)
            v = v * lax.rsqrt(jnp.mean(v * v, axis=-1, keepdims=True) + NORM_EPS)
            n_ref[r] = (v * gain_ref[pl.ds(l, 1)]).astype(jnp.bfloat16)
            return 0
        lax.fori_loop(0, rows // 64, body, 0)

    tile = min(256, width)

    def up_part(k):
        def body(j, _):
            cols = pl.ds(pl.multiple_of(j * tile, tile), tile)
            u = jnp.dot(n_ref[...], wb_ref[k, :, cols], preferred_element_type=jnp.float32)
            a_ref[k, :, cols] = gelu_tanh(u).astype(jnp.bfloat16)
            return 0
        lax.fori_loop(0, width // tile, body, 0)

    def down_part(k):
        def body(j, _):
            cols = pl.ds(pl.multiple_of(j * tile, tile), tile)
            u = jnp.dot(a_ref[k], wb_ref[k, :, cols], preferred_element_type=jnp.float32)
            if k == 0:
                acc_ref[:, cols] = u
            else:
                acc_ref[:, cols] += u
            return 0
        lax.fori_loop(0, d_model // tile, body, 0)

    def residual():
        def body(i, _):
            r = pl.ds(pl.multiple_of(i * 64, 64), 64)
            h_ref[r] = h_ref[r] + acc_ref[r].astype(jnp.bfloat16)
            return 0
        lax.fori_loop(0, rows // 64, body, 0)

    def compute(l, m):
        incoming(7, l, m).wait_recv()
        load(1, l, m).start()
        load(2, l, m).start()
        if m == 0:
            normalize(l)
        for k in range(4):
            if k == 3:
                incoming(8, l, m).wait_recv()
                load(3, l, m).start()
            load(k, l, m).wait()
            (up_part, down_part)[m](k)
        if m == 1:
            residual()
            feat_ref[l // per_feat] = h_ref[...]

    vocab = hs_ref.shape[1]
    v_chunk = hb_ref.shape[2]
    n_v = pl.cdiv(vocab, v_chunk)
    v_tail = vocab - (n_v - 1) * v_chunk

    def load_head(t, slot, act):
        def go(width):
            cols = pl.ds(pl.multiple_of(t * v_chunk, 128), width)
            act(pltpu.make_async_copy(hs_ref.at[:, cols], hb_ref.at[slot, :, pl.ds(0, width)], hs_sem.at[slot]))
        if v_tail == v_chunk:
            pl.when(t < n_v)(lambda: go(v_chunk))
        else:
            pl.when(t < n_v - 1)(lambda: go(v_chunk))
            pl.when(t == n_v - 1)(lambda: go(v_tail))

    v_blk = min(512, v_chunk)

    def student_part(t, slot):
        load_head(t, slot, lambda cp: cp.wait())

        def body(j, _):
            cols = pl.ds(pl.multiple_of(j * v_blk, v_blk), v_blk)
            hs = hb_ref[slot, :, cols]
            limit = vocab - t * v_chunk - j * v_blk
            valid = lax.broadcasted_iota(jnp.int32, (1, v_blk), 1) < limit
            logits = jnp.dot(s_ref[...], hs, preferred_element_type=jnp.float32)
            logits = jnp.where(valid, logits, -jnp.inf)
            m_old = m_ref[...]
            m_new = jnp.maximum(m_old, jnp.max(logits, axis=1, keepdims=True))
            scale = jnp.exp(m_old - m_new)
            e = jnp.exp(logits - m_new)
            m_ref[...] = m_new
            z_ref[...] = z_ref[...] * scale + jnp.sum(e, axis=1, keepdims=True)
            part = lax.dot_general(e.astype(jnp.bfloat16), hs, (((1,), (1,)), ((), ())),
                                   preferred_element_type=jnp.float32)
            ds_ref[...] = ds_ref[...] * scale + part
            return 0

        n_blk = (jnp.minimum(v_chunk, vocab - t * v_chunk) + v_blk - 1) // v_blk

        @pl.when(t < n_v)
        def _():
            lax.fori_loop(0, n_blk, body, 0)

    m_ref[...] = jnp.full_like(m_ref, -jnp.inf)
    z_ref[...] = jnp.zeros_like(z_ref)
    ds_ref[...] = jnp.zeros_like(ds_ref)
    hb_ref[...] = jnp.zeros_like(hb_ref)
    load_head(0, 0, lambda cp: cp.start())

    barrier = pltpu.get_barrier_semaphore()
    for dev in (x_peer, y_peer, z_peer, mate):
        pl.semaphore_signal(barrier, inc=1, device_id=dev, device_id_type=MESH)
    h_ref[...] = x_ref[...]
    pl.semaphore_wait(barrier, 4)

    for l in range(3):
        for m in range(2):
            send_x(l, m)
            if l == 0:
                outgoing(7, l, m).start()
    load(0, 0, 0).start()
    hop_a(0, 0)
    hop_b(0, 0)
    hop_a(0, 1)
    hop_c(0, 0)
    hop_b(0, 1)
    hop_a(1, 0)

    def layer(l, _):
        for m in range(2):
            guarded(send_x, l + 3, m, n_layers)
            guarded(lambda a, b: outgoing(7, a, b).start(), l + 1, m, n_layers)
            nxt = (l, 1) if m == 0 else (l + 1, 0)
            guarded(hop_c, nxt[0], nxt[1], n_layers)
            compute(l, m)
            guarded(lambda a, b: load(0, a, b).start(), nxt[0], nxt[1], n_layers)
            guarded(hop_b, l + 1, m, n_layers)
            t = 2 * l + m
            load_head(t + 1, 1 - m, lambda cp: cp.start())
            student_part(t, m)
            nxt = (l + 1, 1) if m == 0 else (l + 2, 0)
            guarded(hop_a, nxt[0], nxt[1], n_layers)
        return 0

    lax.fori_loop(0, n_layers, layer, 0)
    lse_ref[...] = m_ref[...] + jnp.log(z_ref[...])
    ds_ref[...] = ds_ref[...] / z_ref[...]

    def drain(l, _):
        for m in range(2):
            for stage in range(9):
                outgoing(stage, l, m).wait_send()
        return 0

    lax.fori_loop(0, n_layers, drain, 0)


def direct_rows(d_model):
    return d_model - 8 * seed_rows(d_model)


def seed_rows(d_model):
    return max(16, (d_model // 9) // 16 * 16)


def run_teacher(x_teach, w_up_t, w_down_t, gain_t, n_feat, s_own, head_s):
    n_layers, d_model, width = w_up_t.shape
    rows = x_teach.shape[0] * x_teach.shape[1]
    x_flat = x_teach.reshape(rows, d_model)
    any_spec = pl.BlockSpec(memory_space=pl.ANY)
    vmem_spec = pl.BlockSpec(memory_space=pltpu.VMEM)
    n_ticks = 2 * n_layers
    d_stud, vocab = head_s.shape
    v_chunk = stud_chunk(vocab)
    feat, lse_s, in_grad_s, _, _ = pl.pallas_call(
        functools.partial(teacher_kernel, n_layers),
        name='teacher',
        out_shape=(jax.ShapeDtypeStruct((n_feat, rows, d_model), jnp.bfloat16),
                   jax.ShapeDtypeStruct((rows, 1), jnp.float32),
                   jax.ShapeDtypeStruct((rows, d_stud), jnp.float32),
                   jax.ShapeDtypeStruct((3, n_layers, d_model, width), jnp.bfloat16),
                   jax.ShapeDtypeStruct((3, n_layers, width, d_model), jnp.bfloat16)),
        in_specs=[vmem_spec, vmem_spec, vmem_spec, any_spec, any_spec, any_spec],
        out_specs=(vmem_spec, vmem_spec, vmem_spec, any_spec, any_spec),
        scratch_shapes=[
            pltpu.VMEM((rows, d_model), jnp.bfloat16),
            pltpu.VMEM((rows, d_model), jnp.bfloat16),
            pltpu.VMEM((4, rows, width), jnp.bfloat16),
            pltpu.VMEM((rows, d_model), jnp.float32),
            pltpu.VMEM((4, d_model, width), jnp.bfloat16),
            pltpu.VMEM((2, d_stud, v_chunk), jnp.bfloat16),
            pltpu.VMEM((rows, 1), jnp.float32),
            pltpu.VMEM((rows, 1), jnp.float32),
            pltpu.SemaphoreType.DMA((4,)),
            pltpu.SemaphoreType.DMA((2,)),
            pltpu.SemaphoreType.DMA((9, n_ticks)),
            pltpu.SemaphoreType.DMA((9, n_ticks)),
        ],
        compiler_params=pltpu.CompilerParams(collective_id=0, has_side_effects=True),
        cost_estimate=pl.CostEstimate(flops=2 * rows * d_model * width * 4 * 2 * n_layers,
                                      bytes_accessed=8 * n_layers * d_model * width * 2,
                                      transcendentals=rows * width * 4 * n_layers),
    )(x_flat, gain_t, s_own, w_up_t, w_down_t, head_s)
    return feat, lse_s, in_grad_s


def head_chunk(vocab_part):
    return 512 if vocab_part > 4096 else 128


def grad_chunk(vocab_part):
    return 256 if vocab_part > 4096 else 128


def stats_kernel(vocab_part, h_ref, wt_hbm, ws_ref, fn_hbm, lse_ref, dt_ref,
                 fn_ref, wt_ref, la_ref, lb_ref, e_ref, sc_ref, m_ref, z_ref, acc_ref, got_ref,
                 load_sem, out_sem, send_sem, recv_sem):
    rows, d_model = h_ref.shape
    d_stud, padded = ws_ref.shape
    chunk = la_ref.shape[1]
    n_chunks = padded // chunk
    width = acc_ref.shape[2]
    dp, tp = lax.axis_index('dp'), lax.axis_index('tp')
    x, c = tp // 2, tp % 2
    tp_m, tp_x, tp_xm = x * 2 + 1 - c, (1 - x) * 2 + c, (1 - x) * 2 + 1 - c
    peers = ((dp, tp_m), (dp, tp_x), (dp, tp_xm))
    tail = vocab_part - (n_chunks - 1) * chunk

    def copy(stage, src, dst, dev):
        return pltpu.make_async_remote_copy(src, dst, send_sem.at[stage], recv_sem.at[stage],
                                            device_id=dev, device_id_type=MESH)

    to_mate = copy(0, fn_ref.at[tp], fn_ref.at[tp], peers[0])
    to_x = copy(1, fn_ref.at[tp], fn_ref.at[tp], peers[1])
    relay = copy(2, fn_ref.at[tp_x], fn_ref.at[tp_x], peers[0])
    from_mate = copy(0, fn_ref.at[tp_m], fn_ref.at[tp_m], peers[0])
    from_x = copy(1, fn_ref.at[tp_x], fn_ref.at[tp_x], peers[1])
    from_relay = copy(2, fn_ref.at[tp_xm], fn_ref.at[tp_xm], peers[0])
    back = [copy(3 + i, acc_ref.at[1 + i], got_ref.at[i], peers[i]) for i in range(3)]

    def load(j, size):
        r = pl.ds(pl.multiple_of(j * chunk, 16), size)
        return pltpu.make_async_copy(wt_hbm.at[r], wt_ref.at[r], load_sem.at[j])

    def load_wait(j):
        if tail == chunk:
            load(j, chunk).wait()
        else:
            pl.when(j < n_chunks - 1)(lambda: load(j, chunk).wait())
            pl.when(j == n_chunks - 1)(lambda: load(j, tail).wait())

    barrier = pltpu.get_barrier_semaphore()
    for dev in peers:
        pl.semaphore_signal(barrier, inc=1, device_id=dev, device_id_type=MESH)

    def load_start(j, _):
        load(j, chunk).start()
        return 0

    lax.fori_loop(0, n_chunks - 1, load_start, 0)
    load(n_chunks - 1, tail).start()
    if tail < chunk:
        wt_ref[pl.ds(vocab_part, chunk - tail)] = jnp.zeros((chunk - tail, d_model), jnp.bfloat16)

    def normalize(i, _):
        r = pl.ds(pl.multiple_of(i * 64, 64), 64)
        v = h_ref[r].astype(jnp.float32)
        v = v * lax.rsqrt(jnp.mean(v * v, axis=-1, keepdims=True) + NORM_EPS)
        fn_ref[tp, r] = v.astype(jnp.bfloat16)
        return 0

    lax.fori_loop(0, rows // 64, normalize, 0)
    m_ref[...] = jnp.full_like(m_ref, -jnp.inf)
    z_ref[...] = jnp.zeros_like(z_ref)
    acc_ref[...] = jnp.zeros_like(acc_ref)
    pl.semaphore_wait(barrier, 3)
    to_x.start()
    to_mate.start()

    def logits(q, j, buf, first):
        if first:
            load_wait(j)
        w = wt_ref[pl.ds(pl.multiple_of(j * chunk, chunk), chunk)]
        buf[...] = lax.dot_general(fn_ref[q], w, (((1,), (1,)), ((), ())), preferred_element_type=jnp.float32)

    def fold(g, j, buf):
        ws = ws_ref[:, pl.ds(pl.multiple_of(j * chunk, chunk), chunk)]
        valid = lax.broadcasted_iota(jnp.int32, (1, chunk), 1) < vocab_part - j * chunk
        for i in range(rows // 64):
            r = pl.ds(i * 64, 64)
            v = jnp.where(valid, buf[r], -jnp.inf)
            m_old = m_ref[g, r]
            m_new = jnp.maximum(m_old, jnp.max(v, axis=1, keepdims=True))
            scale = jnp.exp(m_old - m_new)
            e = jnp.exp(v - m_new)
            m_ref[g, r] = m_new
            z_ref[g, r] = z_ref[g, r] * scale + jnp.sum(e, axis=1, keepdims=True)
            sc_ref[r] = scale
            e_ref[r] = e.astype(jnp.bfloat16)
        part = lax.dot_general(e_ref[...], ws, (((1,), (1,)), ((), ())), preferred_element_type=jnp.float32)
        acc_ref[g, :, pl.ds(0, d_stud)] = acc_ref[g, :, pl.ds(0, d_stud)] * sc_ref[...] + part

    def group(g, q, first=False):
        logits(q, 0, la_ref, first)

        def pair(i, _):
            logits(q, 2 * i + 1, lb_ref, first)
            fold(g, 2 * i, la_ref)
            logits(q, 2 * i + 2, la_ref, first)
            fold(g, 2 * i + 1, lb_ref)
            return 0

        n_pairs = (n_chunks - 1) // 2
        lax.fori_loop(0, n_pairs, pair, 0)
        if n_chunks % 2:
            fold(g, n_chunks - 1, la_ref)
        else:
            logits(q, n_chunks - 1, lb_ref, first)
            fold(g, n_chunks - 2, la_ref)
            fold(g, n_chunks - 1, lb_ref)
        lane = lax.broadcasted_iota(jnp.int32, (1, 128), 1)
        last = pl.ds(width - 128, 128)
        v = jnp.where(lane == 127, m_ref[g], acc_ref[g, :, last])
        acc_ref[g, :, last] = jnp.where(lane == 126, z_ref[g], v)

    group(0, tp, True)
    from_mate.wait_recv()
    group(1, tp_m)
    from_x.wait_recv()
    relay.start()
    back[0].start()
    group(2, tp_x)
    from_relay.wait_recv()
    keep = pltpu.make_async_copy(fn_ref, fn_hbm, out_sem)
    keep.start()
    back[1].start()
    group(3, tp_xm)
    for b in back:
        if b is back[2]:
            b.start()
        b.wait_recv()

    def combine(i, _):
        r = pl.ds(pl.multiple_of(i * 64, 64), 64)
        last = pl.ds(width - 128, 128)
        tails = [acc_ref[0, r, last]] + [got_ref[k, r, last] for k in range(3)]
        peaks = [v[:, 127:128] for v in tails]
        peak = jnp.maximum(jnp.maximum(peaks[0], peaks[1]), jnp.maximum(peaks[2], peaks[3]))
        scales = [jnp.exp(p - peak) for p in peaks]
        total = sum(v[:, 126:127] * s for v, s in zip(tails, scales))
        lse_ref[r] = peak + jnp.log(total)
        cols = pl.ds(0, d_stud)
        num = acc_ref[0, r, cols] * scales[0]
        for k in range(3):
            num = num + got_ref[k, r, cols] * scales[k + 1]
        dt_ref[r] = num / total
        return 0

    lax.fori_loop(0, rows // 64, combine, 0)
    keep.wait()
    for cp in (to_mate, to_x, relay, *back):
        cp.wait_send()


def head_stats(h_own, head_rows, head_cols, vocab_part, tp_size):
    rows, d_model = h_own.shape
    d_stud, padded = head_cols.shape
    chunk = head_chunk(vocab_part)
    width = pl.cdiv(d_stud + 2, 128) * 128
    any_spec = pl.BlockSpec(memory_space=pl.ANY)
    vmem_spec = pl.BlockSpec(memory_space=pltpu.VMEM)
    return pl.pallas_call(
        functools.partial(stats_kernel, vocab_part),
        name='head_stats',
        out_shape=(jax.ShapeDtypeStruct((tp_size, rows, d_model), jnp.bfloat16),
                   jax.ShapeDtypeStruct((rows, 1), jnp.float32),
                   jax.ShapeDtypeStruct((rows, d_stud), jnp.float32)),
        in_specs=[vmem_spec, any_spec, vmem_spec],
        out_specs=(any_spec, vmem_spec, vmem_spec),
        scratch_shapes=[
            pltpu.VMEM((tp_size, rows, d_model), jnp.bfloat16),
            pltpu.VMEM((padded, d_model), jnp.bfloat16),
            pltpu.VMEM((rows, chunk), jnp.float32),
            pltpu.VMEM((rows, chunk), jnp.float32),
            pltpu.VMEM((rows, chunk), jnp.bfloat16),
            pltpu.VMEM((rows, 1), jnp.float32),
            pltpu.VMEM((tp_size, rows, 1), jnp.float32),
            pltpu.VMEM((tp_size, rows, 1), jnp.float32),
            pltpu.VMEM((tp_size, rows, width), jnp.float32),
            pltpu.VMEM((tp_size - 1, rows, width), jnp.float32),
            pltpu.SemaphoreType.DMA((padded // chunk,)),
            pltpu.SemaphoreType.DMA,
            pltpu.SemaphoreType.DMA((6,)),
            pltpu.SemaphoreType.DMA((6,)),
        ],
        compiler_params=pltpu.CompilerParams(collective_id=2, has_side_effects=True),
        cost_estimate=pl.CostEstimate(flops=2 * tp_size * rows * vocab_part * (d_model + d_stud),
                                      bytes_accessed=2 * vocab_part * (d_model + d_stud),
                                      transcendentals=tp_size * rows * vocab_part),
    )(h_own, head_rows, head_cols)


HEAD_STAGES = 9


def head_grad_kernel(vocab_part, n_chunks, kl_coef, fn_ref, s_ref, st_ref, lt_ref, ls_ref, wt_ref, ws_ref, out_ref,
                     d_ref, part_ref, yb_ref, nb_ref, fb_ref, kl_ref, copy_sem, send_sem, recv_sem):
    step = pl.program_id(0)
    rows, chunk = fn_ref.shape[0], wt_ref.shape[0]
    d_stud = st_ref.shape[0]
    d_pad = part_ref.shape[1]
    half, quart, eighth = d_pad // 2, d_pad // 4, d_pad // 8
    blk = min(256, rows)
    dp, tp = lax.axis_index('dp'), lax.axis_index('tp')
    z, y = dp // 2, dp % 2
    x, c = tp // 2, tp % 2
    zz, zh = z % 2, z // 2
    tp_x = (1 - x) * 2 + c
    x_peer = (dp, tp_x)
    mate = (dp, x * 2 + 1 - c)
    y_peer = (z * 2 + 1 - y, tp)
    near = ((z + 1 - 2 * zz) * 2 + y, tp)
    far = (((1 - zh) * 2 + zz) * 2 + y, tp)

    def span(yy, n=None, f=None):
        start, size = yy * half, half
        if n is not None:
            start, size = start + n * quart, quart
        if f is not None:
            start, size = start + f * eighth, eighth
        return pl.ds(pl.multiple_of(start, 8), size)

    def cols(i):
        return pl.ds(pl.multiple_of(i * chunk, chunk), chunk)

    def copy(stage, i, src, dst, dev):
        return pltpu.make_async_remote_copy(src, dst, send_sem.at[stage, i], recv_sem.at[stage, i],
                                            device_id=dev, device_id_type=MESH)

    def outgoing(stage, i):
        g = out_ref.at[tp]
        if stage == 0:
            return copy(0, i, part_ref.at[i, span(1 - y)], yb_ref.at[i], y_peer)
        if stage == 1:
            return copy(1, i, part_ref.at[i, span(y, 1 - zz)], nb_ref.at[i], near)
        if stage == 2:
            return copy(2, i, part_ref.at[i, span(y, zz, 1 - zh)], fb_ref.at[i], far)
        if stage == 3:
            r = span(y, zz, zh)
            return copy(3, i, part_ref.at[i, r], g.at[r, cols(i)], far)
        if stage == 4:
            r = span(y, zz)
            return copy(4, i, g.at[r, cols(i)], g.at[r, cols(i)], near)
        if stage == 5:
            r = span(y)
            return copy(5, i, g.at[r, cols(i)], g.at[r, cols(i)], y_peer)
        if stage == 6:
            return copy(6, i, g.at[:, cols(i)], g.at[:, cols(i)], x_peer)
        if stage == 7:
            return copy(7, i, g.at[:, cols(i)], g.at[:, cols(i)], mate)
        gx = out_ref.at[tp_x]
        return copy(8, i, gx.at[:, cols(i)], gx.at[:, cols(i)], mate)

    def incoming(stage, i):
        g = out_ref.at[tp]
        if stage < 3:
            ref = (yb_ref, nb_ref, fb_ref)[stage].at[i]
        elif stage < 6:
            r = (span(y, zz, 1 - zh), span(y, 1 - zz), span(1 - y))[stage - 3]
            ref = g.at[r, cols(i)]
        elif stage == 6:
            ref = out_ref.at[tp_x, :, cols(i)]
        elif stage == 7:
            ref = out_ref.at[x * 2 + 1 - c, :, cols(i)]
        else:
            ref = out_ref.at[(1 - x) * 2 + 1 - c, :, cols(i)]
        return copy(stage, i, ref, ref, mate)

    def keep(i):
        r = span(y, zz, zh)
        return pltpu.make_async_copy(part_ref.at[i, r], out_ref.at[tp, r, cols(i)], copy_sem.at[i])

    def compute(masked):
        if masked:
            valid = step * chunk + lax.broadcasted_iota(jnp.int32, (1, chunk), 1) < vocab_part

        def body(i, _):
            r = pl.ds(pl.multiple_of(i * blk, blk), blk)
            lt = lax.dot_general(fn_ref[r], wt_ref[...], (((1,), (1,)), ((), ())), preferred_element_type=jnp.float32)
            ls = jnp.dot(s_ref[r], ws_ref[...], preferred_element_type=jnp.float32)
            log_t = lt - jnp.concatenate([lt_ref[r]] * (chunk // 128), axis=1)
            log_s = ls - jnp.concatenate([ls_ref[r]] * (chunk // 128), axis=1)
            prob_t = jnp.exp(log_t)
            diff = kl_coef * (jnp.exp(log_s) - prob_t)
            kl = prob_t * (log_t - log_s)
            if masked:
                diff = jnp.where(valid, diff, 0.0)
                kl = jnp.where(valid, kl, 0.0)
            d_ref[r] = diff.astype(jnp.bfloat16)
            kl = jnp.sum(kl.reshape(blk // 8, 8, chunk), axis=0)
            kl_ref[...] += sum(kl[:, k * 128:(k + 1) * 128] for k in range(chunk // 128))
            return 0

        lax.fori_loop(0, rows // blk, body, 0)
        grad = jnp.dot(st_ref[...], d_ref[...], preferred_element_type=jnp.float32)
        part_ref[step, pl.ds(0, d_stud)] = grad
        extra = pl.ds(d_stud, 8)
        part_ref[step, extra] = jnp.zeros((8, chunk), jnp.float32)
        part_ref[step, extra, pl.ds(0, 128)] = kl_ref[...]

    @pl.when(step == 0)
    def _():
        kl_ref[...] = jnp.zeros_like(kl_ref)
        barrier = pltpu.get_barrier_semaphore()
        for dev in (x_peer, y_peer, near, far, mate):
            pl.semaphore_signal(barrier, inc=1, device_id=dev, device_id_type=MESH)
        pl.semaphore_wait(barrier, 5)

    if vocab_part % chunk == 0:
        pl.when(step < n_chunks)(lambda: compute(False))
    else:
        pl.when(step < n_chunks - 1)(lambda: compute(False))
        pl.when(step == n_chunks - 1)(lambda: compute(True))

    def lagged(lag, fn):
        i = step - lag
        pl.when((i >= 0) & (i < n_chunks))(lambda: fn(i))

    def add(stage, rng, buf):
        def fn(i):
            incoming(stage, i).wait_recv()
            part_ref[i, rng] += buf[i]
        return fn

    lagged(1, add(0, span(y), yb_ref))
    lagged(2, add(1, span(y, zz), nb_ref))
    lagged(3, add(2, span(y, zz, zh), fb_ref))

    def start_y(i):
        outgoing(0, i).start()

    def start_near(i):
        outgoing(1, i).start()

    def start_far(i):
        outgoing(2, i).start()

    def start_back_far(i):
        outgoing(3, i).start()
        keep(i).start()

    def start_back_near(i):
        incoming(3, i).wait_recv()
        keep(i).wait()
        outgoing(4, i).start()

    def start_back_y(i):
        incoming(4, i).wait_recv()
        outgoing(5, i).start()

    def start_out(i):
        incoming(5, i).wait_recv()
        outgoing(6, i).start()
        outgoing(7, i).start()

    def start_relay(i):
        incoming(6, i).wait_recv()
        outgoing(8, i).start()

    def finish(i):
        incoming(7, i).wait_recv()
        incoming(8, i).wait_recv()

    for lag, fn in ((0, start_y), (1, start_near), (2, start_far), (3, start_back_far), (4, start_back_near),
                    (5, start_back_y), (6, start_out), (7, start_relay), (8, finish)):
        lagged(lag, fn)

    @pl.when(step == pl.num_programs(0) - 1)
    def _():
        def drain(i, _):
            for stage in range(HEAD_STAGES):
                outgoing(stage, i).wait_send()
            return 0
        lax.fori_loop(0, n_chunks, drain, 0)


def head_grads(full_norm, stud_full, log_t, log_s, head_rows, head_cols, kl_coef, tp_size):
    rows, d_model = full_norm.shape
    d_stud = stud_full.shape[1]
    vocab_part = head_rows.shape[0]
    chunk = grad_chunk(vocab_part)
    n_chunks = pl.cdiv(vocab_part, chunk)
    d_pad = pl.cdiv(d_stud + 8, 64) * 64
    whole = lambda shape: pl.BlockSpec(shape, lambda i: (0, 0), pipeline_mode=pl.Buffered(1))
    return pl.pallas_call(
        functools.partial(head_grad_kernel, vocab_part, n_chunks, kl_coef),
        name='head_grads',
        grid=(n_chunks + 9,),
        out_shape=jax.ShapeDtypeStruct((tp_size, d_pad, n_chunks * chunk), jnp.float32),
        in_specs=[whole((rows, d_model)), whole((rows, d_stud)), whole((d_stud, rows)),
                  whole((rows, 128)), whole((rows, 128)),
                  pl.BlockSpec((chunk, d_model), lambda i: (jnp.minimum(i, n_chunks - 1), 0)),
                  pl.BlockSpec((d_stud, chunk), lambda i: (0, jnp.minimum(i, n_chunks - 1)))],
        out_specs=pl.BlockSpec(memory_space=pl.ANY),
        scratch_shapes=[
            pltpu.VMEM((rows, chunk), jnp.bfloat16),
            pltpu.VMEM((n_chunks, d_pad, chunk), jnp.float32),
            pltpu.VMEM((n_chunks, d_pad // 2, chunk), jnp.float32),
            pltpu.VMEM((n_chunks, d_pad // 4, chunk), jnp.float32),
            pltpu.VMEM((n_chunks, d_pad // 8, chunk), jnp.float32),
            pltpu.VMEM((8, 128), jnp.float32),
            pltpu.SemaphoreType.DMA((n_chunks,)),
            pltpu.SemaphoreType.DMA((HEAD_STAGES, n_chunks)),
            pltpu.SemaphoreType.DMA((HEAD_STAGES, n_chunks)),
        ],
        compiler_params=pltpu.CompilerParams(collective_id=1, has_side_effects=True),
        cost_estimate=pl.CostEstimate(flops=200 * 10**9, bytes_accessed=2 * vocab_part * (d_model + d_stud),
                                      transcendentals=2 * rows * vocab_part),
    )(full_norm, stud_full, stud_full.T, jnp.broadcast_to(log_t[:, None], (rows, 128)),
      jnp.broadcast_to(log_s[:, None], (rows, 128)), head_rows, head_cols)


def join_kernel(vocab_part, in_ref, out_ref):
    out_ref[...] = jnp.concatenate([in_ref[q, :, :vocab_part] for q in range(in_ref.shape[0])], axis=1)


def join_quarters(parts, d_stud, vocab_part):
    n_parts, _, padded = parts.shape
    blk = 24 if d_stud % 24 == 0 else 8
    return pl.pallas_call(
        functools.partial(join_kernel, vocab_part),
        name='join_quarters',
        grid=(d_stud // blk,),
        out_shape=jax.ShapeDtypeStruct((d_stud, n_parts * vocab_part), jnp.float32),
        in_specs=[pl.BlockSpec((n_parts, blk, padded), lambda i: (0, i, 0))],
        out_specs=pl.BlockSpec((blk, n_parts * vocab_part), lambda i: (i, 0)),
        cost_estimate=pl.CostEstimate(flops=d_stud * n_parts * vocab_part, transcendentals=0,
                                      bytes_accessed=8 * d_stud * n_parts * vocab_part),
    )(parts)


def solution(mesh):
    dp_size = mesh.shape['dp']
    tp_size = mesh.shape['tp']

    def local_step(x_teach, x_stud, w_up_t, w_down_t, gain_t, head_t, w_up_s, w_down_s, gain_s, proj_s, head_s):
        n_feat = w_up_s.shape[0]
        d_stud, d_teach = x_stud.shape[2], x_teach.shape[2]
        vocab_part = head_t.shape[1]
        n_own = x_teach.shape[0] * x_teach.shape[1]
        n_tokens = n_own * dp_size * tp_size
        feat_coef = 1.0 / (n_feat * n_tokens * d_teach)
        kl_coef = 1.0 / n_tokens
        tp_idx = lax.axis_index('tp')
        x_stud = lax.all_to_all(x_stud, 'tp', 1, 0, tiled=True).reshape(1, n_own, d_stud)
        saved_acts = student_forward(x_stud, w_up_s, w_down_s, gain_s)
        head_in = saved_acts[-1][7].reshape(n_own, d_stud)
        stud_full = lax.all_gather(head_in, 'tp', axis=0, tiled=True)
        feats, lse_s, in_grad_s = run_teacher(x_teach, w_up_t, w_down_t, gain_t, n_feat, head_in, head_s)
        head_cols = lax.dynamic_slice_in_dim(head_s, tp_idx * vocab_part, vocab_part, axis=1)
        padded = pl.cdiv(vocab_part, head_chunk(vocab_part)) * head_chunk(vocab_part)
        head_cols = jnp.pad(head_cols, ((0, 0), (0, padded - vocab_part)))
        head_rows = head_t.T
        err_grads, err_total, grad_proj = student_errors(saved_acts, proj_s, feats[:, None], feat_coef)
        h_own, grad_proj, stud_full = lax.optimization_barrier((feats[-1], grad_proj, stud_full))
        grad_proj = lax.psum(grad_proj, ('dp', 'tp'))
        full_norm, lse_t, in_grad_t = head_stats(h_own, head_rows, head_cols, vocab_part, tp_size)
        log_norms = lax.all_gather(jnp.concatenate([lse_t, lse_s], axis=1).T, 'tp', axis=0)
        head_in_grad = (kl_coef * (in_grad_s - in_grad_t)).reshape(x_stud.shape)
        grad_up, grad_down, grad_gain = student_backward(saved_acts, w_up_s, w_down_s, gain_s, proj_s, err_grads, head_in_grad)
        extra = jnp.stack([grad_gain, jnp.full_like(grad_gain, feat_coef * err_total)], axis=-1)
        grad_up = jnp.concatenate([grad_up, extra], axis=-1)
        log_norms, grad_up, grad_down, grad_proj = lax.optimization_barrier((log_norms, grad_up, grad_down, grad_proj))
        grad_up, grad_down = lax.psum((grad_up, grad_down), ('dp', 'tp'))
        log_t, log_s = log_norms[:, 0].reshape(-1), log_norms[:, 1].reshape(-1)
        parts = head_grads(full_norm.reshape(-1, d_teach), stud_full, log_t, log_s, head_rows, head_cols, kl_coef, tp_size)
        head_grad = join_quarters(parts, d_stud, vocab_part)
        last = (pl.cdiv(vocab_part, grad_chunk(vocab_part)) - 1) * grad_chunk(vocab_part)
        kl_sum = jnp.sum(parts[:, d_stud:d_stud + 8, last:last + 128])
        d_ff = w_up_s.shape[2]
        total_loss = grad_up[0, 0, d_ff + 1] + kl_coef * kl_sum
        grad_up, grad_gain = grad_up[..., :d_ff], grad_up[..., d_ff]
        return total_loss, grad_up, grad_down, grad_gain, grad_proj, head_grad

    in_specs = (P('dp', 'tp', None), P(('dp', 'tp'), None, None), P(None, None, 'tp'), P(None, 'tp', None),
                P(), P(None, 'tp'), P(), P(), P(), P(), P())
    out_specs = (P(), P(), P(), P(), P(), P())
    return jax.shard_map(local_step, mesh=mesh, in_specs=in_specs, out_specs=out_specs, check_vma=False)
```
